128 devices in a mesh: bl: 32 (over z_hi, y, x), bp: 4 (over z_lo, core).
Axes of the slice: x: 4, y: 4, z: 4 (z_hi: 2, z_lo: 2; z = z_hi * 2 + z_lo), core: 2. Of those that a mesh axis runs over, the one named last changes fastest.
Arguments:
- inverse_cov: float32 [32, 1024, 1024], P('bl', 'bp'), may hold values from -1 to 12, as said below
- channel_keep_mask: int32 [32, 1024], P('bl'), may hold values 0 or 1
- partner_ids: int32 [32, 2], P('bl'), may hold values from -1 to 31, as said below
- band_starts: int32 [2, 64], replicated, may hold values from 0 to 384
Outputs:
- fisher: float32 [2, 64, 64], P(None, 'bp', 'bl')
The draws below stay inside these ranges and needn't reach their ends.
Inputs may be any that keep to these rules, and one draw needn't show every extreme that they name: partner_ids[i, k] is -1 for an empty slot, else the index of a baseline whose group, its index // 1, lies 1 to 4 groups after the group of baseline i, counted cyclically over the 32 groups; in every draw some baseline has all 2 slots filled. Each inverse_cov[i] is symmetric.
All inputs are finite; a program needn't handle non-finite values. No bound on the sum of `channel_keep_mask` on one device may be relied on, other than what follows from the above.
Results may differ from the reference program's by a relative error of at most 0.0003.
Values sent between devices are 32-bit elements; how exact they have to be, the bound alone decides.
A program may use at most 128 MiB of HBM per device.

```python
from functools import partial
import jax
import jax.numpy as jnp
from jax import lax

CHANNEL_COUNT = 1024
PANEL = 512
BANDPOWER_COUNT = 64
WINDOW_LENGTH = 128
PAIRS_PER_SHARD = 1
ANTENNA_PAIRS = 32
COMPANION_SEATS = 2
GROUP_REACH = 4


def draw_inverse_cov(key, part):
    seed_sequence = jax.random.split(key, 5)
    rough_estimate = jax.random.uniform(seed_sequence[0], (ANTENNA_PAIRS, CHANNEL_COUNT, CHANNEL_COUNT), jnp.float32, -1.0, 1.0)
    coupled = (rough_estimate + jnp.swapaxes(rough_estimate, 1, 2)) * (0.5 / 32.0)
    identity = jnp.eye(CHANNEL_COUNT, dtype=jnp.float32)
    diagonal_entries = jax.random.uniform(seed_sequence[1], (ANTENNA_PAIRS, CHANNEL_COUNT), jnp.float32, 1.0, 2.0)
    channel_weighting = jax.random.uniform(seed_sequence[2], (ANTENNA_PAIRS, CHANNEL_COUNT), jnp.float32, 0.5, 1.5)
    correlation_length = jnp.exp(jax.random.uniform(seed_sequence[3], (ANTENNA_PAIRS,), jnp.float32, jnp.log(CHANNEL_COUNT / 4.0), jnp.log(CHANNEL_COUNT * 1.0)))
    signal_amplitude = jax.random.uniform(seed_sequence[4], (ANTENNA_PAIRS,), jnp.float32, 0.04, 0.1)
    channel_pos = jnp.arange(CHANNEL_COUNT, dtype=jnp.float32)
    spread = jnp.abs(channel_pos[:, None] - channel_pos[None, :])
    smooth = signal_amplitude[:, None, None] * channel_weighting[:, :, None] * channel_weighting[:, None, :] * jnp.exp(-spread[None, :, :] / correlation_length[:, None, None])
    alternating = 1.0 - 2.0 * (jnp.arange(CHANNEL_COUNT, dtype=jnp.int32) % 2).astype(jnp.float32)
    parity = 0.1 * alternating[:, None] * alternating[None, :]
    matrix = coupled * (1.0 - identity) + identity * diagonal_entries[:, :, None] + smooth + parity[None, :, :]
    return matrix


def draw_partner_ids(key, part):
    seed_sequence = jax.random.split(key, 6)
    antenna_pair_sets = ANTENNA_PAIRS // PAIRS_PER_SHARD
    antenna_pair_number = jnp.arange(ANTENNA_PAIRS, dtype=jnp.int32)
    rotation_team = antenna_pair_number // PAIRS_PER_SHARD
    turn_shift = jax.random.randint(seed_sequence[0], (), 0, GROUP_REACH, dtype=jnp.int32)
    phase_bit = jax.random.randint(seed_sequence[1], (), 0, 2, dtype=jnp.int32)
    heaviest_group = jax.random.randint(seed_sequence[2], (), 0, ANTENNA_PAIRS, dtype=jnp.int32)
    additional_step = jax.random.randint(seed_sequence[3], (ANTENNA_PAIRS, COMPANION_SEATS), 0, GROUP_REACH, dtype=jnp.int32)
    team_element = jax.random.randint(seed_sequence[4], (ANTENNA_PAIRS, COMPANION_SEATS), 0, PAIRS_PER_SHARD, dtype=jnp.int32)
    keep_probability = jax.random.randint(seed_sequence[5], (ANTENNA_PAIRS, COMPANION_SEATS), 0, 10, dtype=jnp.int32)
    slot_ids = jnp.arange(COMPANION_SEATS, dtype=jnp.int32)[None, :]
    first_hop = ((rotation_team + turn_shift) % GROUP_REACH)[:, None]
    number_of_hops = 1 + jnp.where(slot_ids == 0, first_hop, additional_step)
    steady = ((rotation_team + phase_bit * GROUP_REACH) // GROUP_REACH % 2 == 0)[:, None] & (slot_ids == 0)
    filled = steady | (keep_probability < 3) | (antenna_pair_number == heaviest_group)[:, None]
    companion_pair = (rotation_team[:, None] + number_of_hops) % antenna_pair_sets * PAIRS_PER_SHARD + team_element
    return jnp.where(filled, companion_pair, -1).astype(jnp.int32)


def touch_ends(result, stream_key, low, top_value):
    shape = result.shape
    spot = [jax.random.randint(jax.random.fold_in(stream_key, axis), (), 0, shape[axis]) for axis in range(len(shape))]
    result = result.at[tuple(spot)].set(low)
    longest = shape.index(max(shape))
    spot[longest] = (spot[longest] + 1) % shape[longest]
    return result.at[tuple(spot)].set(top_value)


def setup_inputs(seed: int = 0) -> dict:
    keys = jax.random.split(jax.random.key(seed), 5)
    inverse_cov = draw_inverse_cov(jax.random.fold_in(keys[4], 71), 0)
    channel_keep_mask = touch_ends((jax.random.randint(keys[1], (ANTENNA_PAIRS, CHANNEL_COUNT), 0, 5) < 4).astype(jnp.int32), jax.random.fold_in(keys[1], 1), 0, 1)
    partner_ids = draw_partner_ids(jax.random.fold_in(keys[4], 71), 0)
    band_starts = touch_ends(jax.random.randint(keys[3], (2, BANDPOWER_COUNT), 0, PANEL - WINDOW_LENGTH + 1), jax.random.fold_in(keys[3], 1), 0, PANEL - WINDOW_LENGTH).astype(jnp.int32)
    return dict(inverse_cov=inverse_cov, channel_keep_mask=channel_keep_mask, partner_ids=partner_ids, band_starts=band_starts)


highest = lax.Precision.HIGHEST


def kernel_stack(first_band, band_count, window):
    channel_pos = jnp.arange(window, dtype=jnp.float32)
    spread = jnp.abs(channel_pos[:, None] - channel_pos[None, :])
    band_ids = first_band + jnp.arange(band_count, dtype=jnp.int32)
    length = 1.0 + (band_ids % 4).astype(jnp.float32)
    return jnp.exp(-spread[None, :, :] / length[:, None, None])


def project(panel_block, starts, kernels):
    window = kernels.shape[1]
    window_rows = jax.vmap(lambda row_start: lax.dynamic_slice_in_dim(panel_block, row_start, window, 0))(starts)
    return jnp.einsum("apq,aqc->apc", kernels, window_rows, precision=highest, preferred_element_type=jnp.float32)


def column_windows(projected, starts, window):
    def one_matrix(matrix):
        return jax.vmap(lambda column_start: lax.dynamic_slice_in_dim(matrix, column_start, window, 1))(starts)
    return jax.vmap(one_matrix)(projected)


def baseline_panels(inverse_cov, channel_keep_mask, index):
    matrix = lax.dynamic_index_in_dim(inverse_cov, index, 0, keepdims=False)
    flag_marks = lax.dynamic_index_in_dim(channel_keep_mask, index, 0, keepdims=False).astype(jnp.float32)
    halves = []
    for half_index in range(2):
        lower = half_index * PANEL
        block_part = matrix[lower:lower + PANEL, lower:lower + PANEL]
        marks_half = flag_marks[lower:lower + PANEL]
        halves.append(block_part * marks_half[:, None] * marks_half[None, :])
    return halves


def pair_fisher(own_rows, partner_rows, starts):
    def one_band(inputs):
        partner_row, band_begin = inputs
        partner_windows = column_windows(partner_row[None], starts, WINDOW_LENGTH)[0]
        own_windows = column_windows(own_rows, band_begin[None], WINDOW_LENGTH)[:, 0]
        return jnp.einsum("bpq,bqp->b", partner_windows, own_windows, precision=highest, preferred_element_type=jnp.float32)
    return lax.map(one_band, (partner_rows, starts))


def slot_fisher(inverse_cov, channel_keep_mask, band_starts, kernels, own_rows, target):
    partner_halves = baseline_panels(inverse_cov, channel_keep_mask, target)
    results = []
    for half_index in range(2):
        partner_rows = project(partner_halves[half_index], band_starts[half_index], kernels)
        results.append(pair_fisher(own_rows[half_index], partner_rows, band_starts[half_index]))
    return jnp.stack(results)


def reference(inverse_cov, channel_keep_mask, partner_ids, band_starts):
    kernels = kernel_stack(0, BANDPOWER_COUNT, WINDOW_LENGTH)

    def accumulate_fisher(index, running_totals):
        own_halves = baseline_panels(inverse_cov, channel_keep_mask, index)
        own_rows = [project(own_halves[half_index], band_starts[half_index], kernels) for half_index in range(2)]
        for slot_index in range(COMPANION_SEATS):
            target = partner_ids[index, slot_index]
            safe_target = jnp.maximum(target, 0).astype(jnp.int32)
            running_totals = running_totals + lax.cond(target >= 0, partial(slot_fisher, inverse_cov, channel_keep_mask, band_starts, kernels, own_rows, safe_target), partial(jnp.zeros, (2, BANDPOWER_COUNT, BANDPOWER_COUNT), jnp.float32))
        return running_totals

    running_totals = lax.fori_loop(0, ANTENNA_PAIRS, accumulate_fisher, jnp.zeros((2, BANDPOWER_COUNT, BANDPOWER_COUNT), jnp.float32))
    return running_totals * (1.0 / (4 * ANTENNA_PAIRS * WINDOW_LENGTH))
```

```python
import functools

import jax
import jax.numpy as jnp
from jax import lax
from jax.experimental import pallas as pl
from jax.experimental.pallas import tpu as pltpu
from jax.sharding import PartitionSpec as P

MESH = pl.DeviceIdType.MESH
F32 = jnp.float32
BF16 = jnp.bfloat16

GROUPS = 32
REACH = 4
PANEL = 512
ROWS = 256
BANDS = 64
WINDOW = 128
CLASSES = 4
CHUNKS = 2
CHUNK_ROWS = ROWS // CHUNKS
SCALE = 1.0 / (4 * GROUPS * WINDOW)


def split(x):
    hi = x.astype(BF16)
    return hi, (x - hi.astype(F32)).astype(BF16)


def mm(a, b):
    return jnp.dot(a, b, preferred_element_type=F32)


def dot3(a, b):
    return mm(a[0], b[0]) + (mm(a[0], b[1]) + mm(a[1], b[0]))


def iota(shape, dim):
    return lax.broadcasted_iota(jnp.int32, shape, dim)


def down(row, count):
    return jnp.transpose(jnp.broadcast_to(row, (128, count)))


def body_kernel(
    inv_ref, mask_ref, partner_ref, start_ref, out_ref,
    own_raw, got, got_mask, toep_hi, toep_lo, edge_hi, edge_lo, win, decay_hi, decay_lo,
    decay_t_hi, decay_t_lo, edge_t_hi, edge_t_lo, win_t, panel_hi, panel_lo, filt, filt_edge,
    outer, outer_decay, mixed, gram, total, mirror,
    sum_x, got_x, sum_y, got_y, sum_z, got_z,
    send_sem, recv_sem, mask_send, mask_recv, sib_sem, own_sem, x_sem, y_sem, z_sem,
):
    me = lax.axis_index("bl")
    part = lax.axis_index("bp")
    half = part // 2
    core = part % 2
    pos_x = me % 4
    pos_y = (me // 4) % 4
    pos_z = me // 16
    first = pl.multiple_of(core * ROWS, ROWS)
    col0 = pl.multiple_of(half * PANEL, PANEL)
    sibling = (me, part + 1 - 2 * core)

    def target(d):
        return ((me + GROUPS - d) % GROUPS, part)

    def source(d):
        return ((me + d) % GROUPS, part)

    def x_peer(e):
        return (me - pos_x + (pos_x + e) % 4, part)

    def y_peer(e):
        return (me - 4 * pos_y + 4 * ((pos_y + e) % 4), part)

    spot = pos_z * 4 + part

    def z_peer(e):
        g = (spot + e) % 8
        return (me % 16 + 16 * (g // 4), g % 4)

    peers = (
        [target(d) for d in range(1, REACH + 1)]
        + [source(d) for d in range(1, REACH + 1)]
        + [x_peer(e) for e in range(1, 4)]
        + [y_peer(e) for e in range(1, 4)]
        + [z_peer(e) for e in range(1, 8)]
    )
    barrier = pltpu.get_barrier_semaphore()
    for peer in peers:
        pl.semaphore_signal(barrier, inc=1, device_id=peer, device_id_type=MESH)

    own_rows = own_raw.at[pl.ds(first, ROWS)]
    own_copy = pltpu.make_async_copy(inv_ref.at[0, :, pl.ds(col0, PANEL)], own_rows, own_sem)
    own_copy.start()
    pl.semaphore_wait(barrier, len(peers))

    sib_copy = pltpu.make_async_remote_copy(
        src_ref=inv_ref.at[0, :, pl.ds(col0, PANEL)], dst_ref=own_rows,
        send_sem=sib_sem.at[0], recv_sem=sib_sem.at[1], device_id=sibling, device_id_type=MESH,
    )
    sib_copy.start()
    mask_copies = []
    for d in range(REACH):
        copy = pltpu.make_async_remote_copy(
            src_ref=mask_ref, dst_ref=got_mask.at[d],
            send_sem=mask_send.at[d], recv_sem=mask_recv.at[d],
            device_id=target(d + 1), device_id_type=MESH,
        )
        copy.start()
        mask_copies.append(copy)
    copies = {}
    for k in range(CHUNKS):
        for d in range(REACH):
            copy = pltpu.make_async_remote_copy(
                src_ref=inv_ref.at[0, pl.ds(k * CHUNK_ROWS, CHUNK_ROWS), pl.ds(col0, PANEL)],
                dst_ref=got.at[d, pl.ds(k * CHUNK_ROWS, CHUNK_ROWS)],
                send_sem=send_sem.at[d, k], recv_sem=recv_sem.at[d, k],
                device_id=target(d + 1), device_id_type=MESH,
            )
            copy.start()
            copies[d, k] = copy

    starts = start_ref[pl.ds(half, 1), :]
    starts2 = jnp.concatenate([starts, starts], axis=1)
    lane = iota((1, 2 * BANDS), 1)
    lane_class = lane % CLASSES
    rate = 1.0 / (1 + lane_class).astype(F32)
    is_left = lane < BANDS
    for r0 in range(0, PANEL, 128):
        pos = iota((128, 2 * BANDS), 0) + r0
        from_start = pos - starts2
        to_end = starts2 + (WINDOW - 1) - pos
        inside = (from_start >= 0) & (to_end >= 0)
        gap = jnp.where(is_left, -from_start, -to_end)
        edge = jnp.where(gap > 0, jnp.exp(-jnp.abs(gap).astype(F32) * rate), 0.0)
        edge_hi[r0 : r0 + 128, :], edge_lo[r0 : r0 + 128, :] = split(edge)
        decay = jnp.where(inside, jnp.exp(-jnp.abs(gap).astype(F32) * rate), 0.0)
        decay_hi[r0 : r0 + 128, :], decay_lo[r0 : r0 + 128, :] = split(decay)
        for l in range(CLASSES):
            one = jnp.where(inside & (lane_class == l), 1.0, 0.0)[:, :BANDS]
            win[l * PANEL + r0 : l * PANEL + r0 + 128, :] = one.astype(BF16)
    starts_t = down(starts2.astype(F32), 2 * BANDS).astype(jnp.int32)
    sub = iota((2 * BANDS, 128), 0)
    sub_class = sub % CLASSES
    rate_t = 1.0 / (1 + sub_class).astype(F32)
    is_left_t = sub < BANDS
    for r0 in range(0, PANEL, 128):
        pos = iota((2 * BANDS, 128), 1) + r0
        from_start = pos - starts_t
        to_end = starts_t + (WINDOW - 1) - pos
        inside = (from_start >= 0) & (to_end >= 0)
        gap = jnp.where(is_left_t, -from_start, -to_end)
        weight = jnp.exp(-jnp.abs(gap).astype(F32) * rate_t)
        edge_t_hi[:, r0 : r0 + 128], edge_t_lo[:, r0 : r0 + 128] = split(
            jnp.where(gap > 0, weight, 0.0)
        )
        decay_t_hi[:, r0 : r0 + 128], decay_t_lo[:, r0 : r0 + 128] = split(
            jnp.where(inside, weight, 0.0)
        )
        for l in range(CLASSES):
            one = jnp.where(inside & (sub_class == l), 1.0, 0.0)[:BANDS, :]
            win_t[l, :, r0 : r0 + 128] = one.astype(BF16)

    def fill(block, carry):
        r0 = pl.multiple_of(block * 128, 128)
        dist = jnp.abs(iota((128, PANEL), 0) + r0 - iota((128, PANEL), 1)).astype(F32)
        for l in range(CLASSES):
            hi, lo = split(jnp.exp(dist * (-1.0 / (1 + l))))
            toep_hi[pl.ds(r0, 128), l * PANEL : (l + 1) * PANEL] = hi
            toep_lo[pl.ds(r0, 128), l * PANEL : (l + 1) * PANEL] = lo
        return carry

    lax.fori_loop(0, PANEL // 128, fill, 0)

    own_copy.wait()
    sib_copy.wait()
    cols = mask_ref[:, pl.ds(col0, PANEL)].astype(F32)
    for r0 in range(0, PANEL, 128):
        marks = down(cols[:, r0 : r0 + 128], 128)
        for c0 in range(0, PANEL, 128):
            block = own_raw[r0 : r0 + 128, c0 : c0 + 128] * marks * cols[:, c0 : c0 + 128]
            panel_hi[r0 : r0 + 128, c0 : c0 + 128], panel_lo[r0 : r0 + 128, c0 : c0 + 128] = split(
                block
            )
    panel = (panel_hi[...], panel_lo[...])
    decays = (decay_hi[...], decay_lo[...])
    for l in range(CLASSES):
        rows = (
            toep_hi[pl.ds(first, ROWS), l * PANEL : (l + 1) * PANEL],
            toep_lo[pl.ds(first, ROWS), l * PANEL : (l + 1) * PANEL],
        )
        out = dot3(rows, panel)
        filt[l] = out
        filt_edge[l] = dot3(split(out), decays)
    outer[...] = dot3((edge_t_hi[...], edge_t_lo[...]), panel)
    outer_decay[...] = dot3(split(outer[...]), decays)

    for d in range(REACH):
        mask_copies[d].wait()
    total[...] = jnp.zeros_like(total)
    gram[...] = jnp.zeros_like(gram)
    mirror[...] = jnp.zeros_like(mirror)
    weights = []
    for d in range(REACH):
        wanted = (me + d + 1) % GROUPS
        weight = 0.0
        for slot in range(2):
            weight = weight + jnp.where(partner_ref[0, slot] == wanted, 1.0, 0.0)
        weights.append(weight)
    for k in range(CHUNKS):
        y0 = k * CHUNK_ROWS
        for d in range(REACH):
            copies[d, k].wait_recv()
        blocks = [0.0] * (PANEL // 128)
        for d in range(REACH):
            row_marks = got_mask[d, :, pl.ds(pl.multiple_of(col0 + first + y0, 128), CHUNK_ROWS)]
            marks = down(row_marks.astype(F32) * weights[d], CHUNK_ROWS)
            cols = got_mask[d, :, pl.ds(col0, PANEL)].astype(F32)
            for c in range(PANEL // 128):
                span = slice(c * 128, c * 128 + 128)
                blocks[c] = blocks[c] + got[d, y0 : y0 + CHUNK_ROWS, span] * marks * cols[:, span]
        rows = split(jnp.concatenate(blocks, axis=1))
        here = pl.ds(pl.multiple_of(first + y0, 128), CHUNK_ROWS)
        decay_t = (decay_t_hi[:, here], decay_t_lo[:, here])
        edges = dot3(rows, (edge_hi[...], edge_lo[...]))
        mirror[...] += dot3(decay_t, split(edges))
        for l in range(CLASSES):
            span = slice(l * PANEL, (l + 1) * PANEL)
            out = dot3(rows, (toep_hi[:, span], toep_lo[:, span]))
            mixed[:, span] = out
            gram[:, span] += dot3(decay_t, split(out))
        acc = jnp.zeros((BANDS, BANDS), F32)
        for lb in range(CLASSES):
            rim = edges * filt_edge[lb, y0 : y0 + CHUNK_ROWS, :]
            sums = -(rim[:, :BANDS] + rim[:, BANDS:])
            for la in range(CLASSES):
                span = slice(la * PANEL, (la + 1) * PANEL)
                hi, lo = split(mixed[:, span] * filt[lb, y0 : y0 + CHUNK_ROWS, :])
                sums = sums + (mm(hi, win[span, :]) + mm(lo, win[span, :]))
            hi, lo = split(sums)
            acc = acc + (mm(win_t[lb, :, here], hi) + mm(win_t[lb, :, here], lo))
        total[...] += acc
    cross = jnp.zeros((2 * BANDS, BANDS), F32)
    for la in range(CLASSES):
        span = slice(la * PANEL, (la + 1) * PANEL)
        hi, lo = split(gram[:, span] * outer[...])
        cross = cross + (mm(hi, win[span, :]) + mm(lo, win[span, :]))
    four = mirror[...] * outer_decay[...]
    fisher = total[...] - cross[:BANDS] - cross[BANDS:]
    fisher = fisher + (four[:BANDS, :BANDS] + four[:BANDS, BANDS:])
    fisher = fisher + (four[BANDS:, :BANDS] + four[BANDS:, BANDS:])
    fisher = fisher * SCALE

    row = iota((BANDS // 2, BANDS), 0)
    owner = (row % 2) * 16 + ((row // 2) % 4) * 4 + row // 8
    col = iota((BANDS // 2, BANDS), 1)
    parts3 = []
    rest = fisher
    for _ in range(3):
        piece = rest.astype(BF16)
        parts3.append(piece)
        rest = rest - piece.astype(F32)
    turned = []
    for side in range(2):
        pick = jnp.where(col == 2 * owner + side, 1.0, 0.0).astype(BF16)
        turned.append(mm(pick, parts3[0]) + mm(pick, parts3[1]) + mm(pick, parts3[2]))
    placed = jnp.concatenate(turned, axis=1)
    for x in range(4):
        sum_x[x] = placed[8 * x : 8 * x + 8]

    x_copies = []
    for e in range(1, 4):
        copy = pltpu.make_async_remote_copy(
            src_ref=sum_x.at[(pos_x + e) % 4], dst_ref=got_x.at[e - 1],
            send_sem=x_sem.at[0, e - 1], recv_sem=x_sem.at[1, e - 1],
            device_id=x_peer(e), device_id_type=MESH,
        )
        copy.start()
        x_copies.append(copy)
    tile = sum_x[pos_x]
    for e in range(3):
        x_copies[e].wait_recv()
        tile = tile + got_x[e]
    sum_y[...] = tile
    y_copies = []
    for e in range(1, 4):
        copy = pltpu.make_async_remote_copy(
            src_ref=sum_y, dst_ref=got_y.at[e - 1],
            send_sem=y_sem.at[0, e - 1], recv_sem=y_sem.at[1, e - 1],
            device_id=y_peer(e), device_id_type=MESH,
        )
        copy.start()
        y_copies.append(copy)
    for e in range(3):
        y_copies[e].wait_recv()
        tile = tile + got_y[e]
    sum_z[...] = tile
    z_copies = []
    for e in range(1, 8):
        copy = pltpu.make_async_remote_copy(
            src_ref=sum_z, dst_ref=got_z.at[e - 1],
            send_sem=z_sem.at[0, e - 1], recv_sem=z_sem.at[1, e - 1],
            device_id=z_peer(e), device_id_type=MESH,
        )
        copy.start()
        z_copies.append(copy)
    halves = [jnp.where(half == h, tile, 0.0) for h in range(2)]
    for e in range(7):
        z_copies[e].wait_recv()
        from_half = ((spot + 7 - e) % 8 % 4) // 2
        for h in range(2):
            halves[h] = halves[h] + jnp.where(from_half == h, got_z[e], 0.0)
    my_row = pos_y * 2 + pos_z
    lanes = iota((16, 128), 1)
    for h in range(2):
        line = jnp.sum(jnp.where(iota((8, 128), 0) == my_row, halves[h], 0.0), axis=0, keepdims=True)
        line = jnp.broadcast_to(line, (16, 128))
        band = 16 * part + iota((16, 128), 0)
        for side in range(2):
            one = jnp.where(lanes == band + side * BANDS, line, 0.0)
            out_ref[h, :, side : side + 1] = jnp.sum(one, axis=1, keepdims=True)

    for copy in list(copies.values()) + x_copies + y_copies + z_copies:
        copy.wait_send()


def body(inverse_cov, channel_keep_mask, partner_ids, band_starts):
    vmem = pltpu.VMEM
    dma = pltpu.SemaphoreType.DMA
    return pl.pallas_call(
        body_kernel,
        out_shape=jax.ShapeDtypeStruct((2, 16, 2), F32),
        in_specs=[
            pl.BlockSpec(memory_space=pl.ANY),
            pl.BlockSpec(memory_space=pltpu.VMEM),
            pl.BlockSpec(memory_space=pltpu.SMEM),
            pl.BlockSpec(memory_space=pltpu.VMEM),
        ],
        out_specs=pl.BlockSpec(memory_space=pltpu.VMEM),
        scratch_shapes=[
            vmem((PANEL, PANEL), F32),
            vmem((REACH, ROWS, PANEL), F32),
            vmem((REACH, 1, 2 * PANEL), jnp.int32),
            vmem((PANEL, CLASSES * PANEL), BF16),
            vmem((PANEL, CLASSES * PANEL), BF16),
            vmem((PANEL, 2 * BANDS), BF16),
            vmem((PANEL, 2 * BANDS), BF16),
            vmem((CLASSES * PANEL, BANDS), BF16),
            vmem((PANEL, 2 * BANDS), BF16),
            vmem((PANEL, 2 * BANDS), BF16),
            vmem((2 * BANDS, PANEL), BF16),
            vmem((2 * BANDS, PANEL), BF16),
            vmem((2 * BANDS, PANEL), BF16),
            vmem((2 * BANDS, PANEL), BF16),
            vmem((CLASSES, BANDS, PANEL), BF16),
            vmem((PANEL, PANEL), BF16),
            vmem((PANEL, PANEL), BF16),
            vmem((CLASSES, ROWS, PANEL), F32),
            vmem((CLASSES, ROWS, 2 * BANDS), F32),
            vmem((2 * BANDS, PANEL), F32),
            vmem((2 * BANDS, 2 * BANDS), F32),
            vmem((CHUNK_ROWS, CLASSES * PANEL), F32),
            vmem((2 * BANDS, CLASSES * PANEL), F32),
            vmem((BANDS, BANDS), F32),
            vmem((2 * BANDS, 2 * BANDS), F32),
            vmem((4, 8, 128), F32),
            vmem((3, 8, 128), F32),
            vmem((8, 128), F32),
            vmem((3, 8, 128), F32),
            vmem((8, 128), F32),
            vmem((7, 8, 128), F32),
            dma((REACH, CHUNKS)),
            dma((REACH, CHUNKS)),
            dma((REACH,)),
            dma((REACH,)),
            dma((2,)),
            dma,
            dma((2, 3)),
            dma((2, 3)),
            dma((2, 7)),
        ],
        compiler_params=pltpu.CompilerParams(
            collective_id=0, has_side_effects=True, vmem_limit_bytes=48 * 1024 * 1024
        ),
    )(inverse_cov, channel_keep_mask, partner_ids, band_starts)


def solution(mesh):
    placed = (P("bl", "bp", None), P("bl", None), P("bl", None), P())
    return jax.shard_map(
        body, mesh=mesh, in_specs=placed, out_specs=P(None, "bp", "bl"), check_vma=False
    )
```

```python
import functools

import jax
import jax.numpy as jnp
from jax import lax
from jax.experimental import pallas as pl
from jax.experimental.pallas import tpu as pltpu
from jax.sharding import PartitionSpec as P

MESH = pl.DeviceIdType.MESH
F32 = jnp.float32
BF16 = jnp.bfloat16

GROUPS = 32
REACH = 4
SENDS = (-1, 2, -3, 4)
BLOCK = 128
GROUPS_OF_BLOCKS = ((0, 2), (2, 2), (4, 1))
PANEL = 512
ROWS = 256
BANDS = 64
WINDOW = 128
CLASSES = 4
SCALE = 1.0 / (4 * GROUPS * WINDOW)


def split(x):
    hi = x.astype(BF16)
    return hi, (x - hi.astype(F32)).astype(BF16)


def mm(a, b):
    return jnp.dot(a, b, preferred_element_type=F32)


def dot3(a, b):
    return mm(a[0], b[0]) + (mm(a[0], b[1]) + mm(a[1], b[0]))


def iota(shape, dim):
    return lax.broadcasted_iota(jnp.int32, shape, dim)


def down(row, count):
    return jnp.transpose(jnp.broadcast_to(row, (128, count)))


def body_kernel(
    inv_ref, mask_hbm, partner_hbm, start_hbm, out_ref,
    mask_ref, partner_ref, start_ref, own_raw, own_pack, got, got_mask, got_partner, row_marks,
    far_sum, got_far, rows_hi, rows_lo,
    toep_hi, toep_lo, edge_hi, edge_lo, win, decay_hi, decay_lo,
    decay_t_hi, decay_t_lo, edge_t_hi, edge_t_lo, win_t, panel_hi, panel_lo, filt, filt_edge,
    outer, outer_decay, mixed, gram, total, mirror,
    sum_x, got_x, sum_y, got_y, sum_z, got_z,
    send_sem, recv_sem, mask_sem, partner_sem, sib_sem, far_sem, own_sem, x_sem, y_sem, z_sem,
):
    me = lax.axis_index("bl")
    part = lax.axis_index("bp")
    half = part // 2
    core = part % 2
    pos_x = me % 4
    pos_y = (me // 4) % 4
    pos_z = me // 16
    first = pl.multiple_of(core * ROWS, ROWS)
    col0 = pl.multiple_of(half * PANEL, PANEL)
    sibling = (me, part + 1 - 2 * core)

    def by_core(zero, one):
        return core * (one - zero) + zero

    def target(d):
        return ((me + GROUPS + SENDS[d]) % GROUPS, part)

    def source(d):
        return ((me + GROUPS - SENDS[d]) % GROUPS, part)

    near = [2 * core, 2 * core + 1]
    far = [by_core(2 + r, 1 - r) for r in range(2)]
    missing = [by_core(3 - r, r) for r in range(2)]
    missing_slot = [by_core(1 - r, r) for r in range(2)]
    pack = [(0, far[0]), (1, far[1]), (0, near[0]), (0, near[1]), (1, near[1])]

    def lanes_of(block):
        return pl.ds(pl.multiple_of(col0 + BLOCK * block, BLOCK), BLOCK)

    def x_peer(e):
        return (me - pos_x + (pos_x + e) % 4, part)

    def y_peer(e):
        return (me - 4 * pos_y + 4 * ((pos_y + e) % 4), part)

    spot = pos_z * 4 + part

    def z_peer(e):
        g = (spot + e) % 8
        return (me % 16 + 16 * (g // 4), g % 4)

    peers = (
        [target(d) for d in range(REACH)]
        + [source(d) for d in range(REACH)]
        + [x_peer(e) for e in range(1, 4)]
        + [y_peer(e) for e in range(1, 4)]
        + [z_peer(e) for e in range(1, 8)]
    )
    barrier = pltpu.get_barrier_semaphore()
    for peer in peers:
        pl.semaphore_signal(barrier, inc=1, device_id=peer, device_id_type=MESH)

    locals_ = [
        pltpu.make_async_copy(
            inv_ref.at[0, BLOCK * r : BLOCK * (r + 1), lanes_of(c)], own_pack.at[p], own_sem.at[p]
        )
        for p, (r, c) in enumerate(pack)
    ]
    own_rows = own_raw.at[pl.ds(first, ROWS)]
    locals_.append(
        pltpu.make_async_copy(inv_ref.at[0, :, pl.ds(col0, PANEL)], own_rows, own_sem.at[5])
    )
    locals_.append(pltpu.make_async_copy(mask_hbm, mask_ref, own_sem.at[6]))
    locals_.append(pltpu.make_async_copy(partner_hbm, partner_ref, own_sem.at[7]))
    locals_.append(pltpu.make_async_copy(start_hbm, start_ref, own_sem.at[8]))
    for copy in locals_:
        copy.start()
    for copy in locals_:
        copy.wait()
    pl.semaphore_wait(barrier, len(peers))

    sib_copy = pltpu.make_async_remote_copy(
        src_ref=own_rows, dst_ref=own_rows,
        send_sem=sib_sem.at[0], recv_sem=sib_sem.at[1], device_id=sibling, device_id_type=MESH,
    )
    sib_copy.start()
    mask_copies = []
    for d in range(REACH):
        pairs = [(mask_ref, got_mask, mask_sem)]
        if SENDS[d] > 0:
            pairs.append((partner_ref, got_partner, partner_sem))
        for src, dst, sem in pairs:
            copy = pltpu.make_async_remote_copy(
                src_ref=src, dst_ref=dst.at[d], send_sem=sem.at[0, d], recv_sem=sem.at[1, d],
                device_id=target(d), device_id_type=MESH,
            )
            copy.start()
            mask_copies.append(copy)
    copies = {}
    for g, (p, count) in enumerate(GROUPS_OF_BLOCKS):
        for d in range(REACH):
            copy = pltpu.make_async_remote_copy(
                src_ref=own_pack.at[pl.ds(p, count)], dst_ref=got.at[d, pl.ds(p, count)],
                send_sem=send_sem.at[d, g], recv_sem=recv_sem.at[d, g],
                device_id=target(d), device_id_type=MESH,
            )
            copy.start()
            copies[d, g] = copy

    starts = start_ref[pl.ds(half, 1), :]
    starts2 = jnp.concatenate([starts, starts], axis=1)
    lane = iota((1, 2 * BANDS), 1)
    lane_class = lane % CLASSES
    rate = 1.0 / (1 + lane_class).astype(F32)
    is_left = lane < BANDS
    for r0 in range(0, PANEL, 128):
        pos = iota((128, 2 * BANDS), 0) + r0
        from_start = pos - starts2
        to_end = starts2 + (WINDOW - 1) - pos
        inside = (from_start >= 0) & (to_end >= 0)
        gap = jnp.where(is_left, -from_start, -to_end)
        edge = jnp.where(gap > 0, jnp.exp(-jnp.abs(gap).astype(F32) * rate), 0.0)
        edge_hi[r0 : r0 + 128, :], edge_lo[r0 : r0 + 128, :] = split(edge)
        decay = jnp.where(inside, jnp.exp(-jnp.abs(gap).astype(F32) * rate), 0.0)
        decay_hi[r0 : r0 + 128, :], decay_lo[r0 : r0 + 128, :] = split(decay)
        for l in range(CLASSES):
            one = jnp.where(inside & (lane_class == l), 1.0, 0.0)[:, :BANDS]
            win[l * PANEL + r0 : l * PANEL + r0 + 128, :] = one.astype(BF16)
    starts_t = down(starts2.astype(F32), 2 * BANDS).astype(jnp.int32)
    sub = iota((2 * BANDS, 128), 0)
    sub_class = sub % CLASSES
    rate_t = 1.0 / (1 + sub_class).astype(F32)
    is_left_t = sub < BANDS
    for r0 in range(0, PANEL, 128):
        pos = iota((2 * BANDS, 128), 1) + r0
        from_start = pos - starts_t
        to_end = starts_t + (WINDOW - 1) - pos
        inside = (from_start >= 0) & (to_end >= 0)
        gap = jnp.where(is_left_t, -from_start, -to_end)
        weight = jnp.exp(-jnp.abs(gap).astype(F32) * rate_t)
        edge_t_hi[:, r0 : r0 + 128], edge_t_lo[:, r0 : r0 + 128] = split(
            jnp.where(gap > 0, weight, 0.0)
        )
        decay_t_hi[:, r0 : r0 + 128], decay_t_lo[:, r0 : r0 + 128] = split(
            jnp.where(inside, weight, 0.0)
        )
        for l in range(CLASSES):
            one = jnp.where(inside & (sub_class == l), 1.0, 0.0)[:BANDS, :]
            win_t[l, :, r0 : r0 + 128] = one.astype(BF16)

    def fill(block, carry):
        r0 = pl.multiple_of(block * 128, 128)
        dist = jnp.abs(iota((128, PANEL), 0) + r0 - iota((128, PANEL), 1)).astype(F32)
        for l in range(CLASSES):
            hi, lo = split(jnp.exp(dist * (-1.0 / (1 + l))))
            toep_hi[pl.ds(r0, 128), l * PANEL : (l + 1) * PANEL] = hi
            toep_lo[pl.ds(r0, 128), l * PANEL : (l + 1) * PANEL] = lo
        return carry

    lax.fori_loop(0, PANEL // 128, fill, 0)

    sib_copy.wait()
    cols = mask_ref[:, pl.ds(col0, PANEL)].astype(F32)
    for r0 in range(0, PANEL, 128):
        marks = down(cols[:, r0 : r0 + 128], 128)
        for c0 in range(0, PANEL, 128):
            block = own_raw[r0 : r0 + 128, c0 : c0 + 128] * marks * cols[:, c0 : c0 + 128]
            panel_hi[r0 : r0 + 128, c0 : c0 + 128], panel_lo[r0 : r0 + 128, c0 : c0 + 128] = split(
                block
            )
    panel = (panel_hi[...], panel_lo[...])
    decays = (decay_hi[...], decay_lo[...])
    for l in range(CLASSES):
        rows = (
            toep_hi[pl.ds(first, ROWS), l * PANEL : (l + 1) * PANEL],
            toep_lo[pl.ds(first, ROWS), l * PANEL : (l + 1) * PANEL],
        )
        out = dot3(rows, panel)
        filt[l] = out
        filt_edge[l] = dot3(split(out), decays)
    outer[...] = dot3((edge_t_hi[...], edge_t_lo[...]), panel)
    outer_decay[...] = dot3(split(outer[...]), decays)

    for copy in mask_copies:
        copy.wait()
    total[...] = jnp.zeros_like(total)
    gram[...] = jnp.zeros_like(gram)
    mirror[...] = jnp.zeros_like(mirror)
    for d in range(REACH):
        if SENDS[d] < 0:
            hits = jnp.where(partner_ref[...] == source(d)[0], 1.0, 0.0)
        else:
            hits = jnp.where(got_partner[d] == me, 1.0, 0.0)
        weight = hits[:, 0:1] + hits[:, 1:2]
        for r in range(2):
            marks = got_mask[d, :, lanes_of(near[r])].astype(F32) * weight
            row_marks[d, r] = down(marks, BLOCK)

    def summed(p):
        r, c = pack[p]
        out = 0.0
        for d in range(REACH):
            cols = got_mask[d, :, lanes_of(c)].astype(F32)
            out = out + got[d, p] * row_marks[d, r] * cols
        return out

    def put(block, value):
        hi, lo = split(value)
        spot = pl.ds(pl.multiple_of(BLOCK * block, BLOCK), BLOCK)
        rows_hi[:, spot] = hi
        rows_lo[:, spot] = lo

    far_copy = pltpu.make_async_remote_copy(
        src_ref=far_sum, dst_ref=got_far,
        send_sem=far_sem.at[0], recv_sem=far_sem.at[1], device_id=sibling, device_id_type=MESH,
    )
    for d in range(REACH):
        copies[d, 0].wait_recv()
    for r in range(2):
        far_sum[r] = summed(r)
    far_copy.start()
    for k in range(2):
        y0 = k * BLOCK
        for d in range(REACH):
            copies[d, k + 1].wait_recv()
        if k == 0:
            far_copy.wait_recv()
        put(far[k], far_sum[k])
        put(missing[k], jnp.transpose(got_far[missing_slot[k]]))
        if k == 0:
            put(near[0], summed(2))
            corner = summed(3)
            put(near[1], corner)
            row_marks[0, 0] = jnp.transpose(corner)
        else:
            put(near[0], row_marks[0, 0])
            put(near[1], summed(4))
        rows = (rows_hi[...], rows_lo[...])
        here = pl.ds(pl.multiple_of(first + y0, BLOCK), BLOCK)
        decay_t = (decay_t_hi[:, here], decay_t_lo[:, here])
        edges = dot3(rows, (edge_hi[...], edge_lo[...]))
        mirror[...] += dot3(decay_t, split(edges))
        for l in range(CLASSES):
            span = slice(l * PANEL, (l + 1) * PANEL)
            out = dot3(rows, (toep_hi[:, span], toep_lo[:, span]))
            mixed[:, span] = out
            gram[:, span] += dot3(decay_t, split(out))
        acc = jnp.zeros((BANDS, BANDS), F32)
        for lb in range(CLASSES):
            rim = edges * filt_edge[lb, y0 : y0 + BLOCK, :]
            sums = -(rim[:, :BANDS] + rim[:, BANDS:])
            for la in range(lb + 1):
                span = slice(la * PANEL, (la + 1) * PANEL)
                hi, lo = split(mixed[:, span] * filt[lb, y0 : y0 + BLOCK, :])
                sums = sums + (mm(hi, win[span, :]) + mm(lo, win[span, :]))
            hi, lo = split(sums)
            acc = acc + (mm(win_t[lb, :, here], hi) + mm(win_t[lb, :, here], lo))
        total[...] += acc
    cross = jnp.zeros((2 * BANDS, BANDS), F32)
    for la in range(CLASSES):
        span = slice(la * PANEL, (la + 1) * PANEL)
        hi, lo = split(gram[:, span] * outer[...])
        cross = cross + (mm(hi, win[span, :]) + mm(lo, win[span, :]))
    four = mirror[...] * outer_decay[...]
    fisher = total[...] - cross[:BANDS] - cross[BANDS:]
    fisher = fisher + (four[:BANDS, :BANDS] + four[:BANDS, BANDS:])
    fisher = fisher + (four[BANDS:, :BANDS] + four[BANDS:, BANDS:])
    row_class = iota((BANDS, BANDS), 0) % CLASSES
    col_class = iota((BANDS, BANDS), 1) % CLASSES
    kept = jnp.where(col_class <= row_class, fisher * SCALE, 0.0)
    wide = jnp.concatenate([kept, jnp.zeros_like(kept)], axis=1)
    turned_over = jnp.transpose(jnp.concatenate([wide, jnp.zeros_like(wide)], axis=0))
    fisher = kept + jnp.where(col_class > row_class, turned_over[:BANDS, :BANDS], 0.0)

    row = iota((BANDS // 2, BANDS), 0)
    owner = (row % 2) * 16 + ((row // 2) % 4) * 4 + row // 8
    col = iota((BANDS // 2, BANDS), 1)
    parts3 = []
    rest = fisher
    for _ in range(3):
        piece = rest.astype(BF16)
        parts3.append(piece)
        rest = rest - piece.astype(F32)
    turned = []
    for side in range(2):
        pick = jnp.where(col == 2 * owner + side, 1.0, 0.0).astype(BF16)
        turned.append(mm(pick, parts3[0]) + mm(pick, parts3[1]) + mm(pick, parts3[2]))
    placed = jnp.concatenate(turned, axis=1)
    for x in range(4):
        sum_x[x] = placed[8 * x : 8 * x + 8]

    x_copies = []
    for e in range(1, 4):
        copy = pltpu.make_async_remote_copy(
            src_ref=sum_x.at[(pos_x + e) % 4], dst_ref=got_x.at[e - 1],
            send_sem=x_sem.at[0, e - 1], recv_sem=x_sem.at[1, e - 1],
            device_id=x_peer(e), device_id_type=MESH,
        )
        copy.start()
        x_copies.append(copy)
    tile = sum_x[pos_x]
    for e in range(3):
        x_copies[e].wait_recv()
        tile = tile + got_x[e]
    sum_y[...] = tile
    y_copies = []
    for e in range(1, 4):
        copy = pltpu.make_async_remote_copy(
            src_ref=sum_y, dst_ref=got_y.at[e - 1],
            send_sem=y_sem.at[0, e - 1], recv_sem=y_sem.at[1, e - 1],
            device_id=y_peer(e), device_id_type=MESH,
        )
        copy.start()
        y_copies.append(copy)
    for e in range(3):
        y_copies[e].wait_recv()
        tile = tile + got_y[e]
    sum_z[...] = tile
    z_copies = []
    for e in range(1, 8):
        copy = pltpu.make_async_remote_copy(
            src_ref=sum_z, dst_ref=got_z.at[e - 1],
            send_sem=z_sem.at[0, e - 1], recv_sem=z_sem.at[1, e - 1],
            device_id=z_peer(e), device_id_type=MESH,
        )
        copy.start()
        z_copies.append(copy)
    halves = [jnp.where(half == h, tile, 0.0) for h in range(2)]
    for e in range(7):
        z_copies[e].wait_recv()
        from_half = ((spot + 7 - e) % 8 % 4) // 2
        for h in range(2):
            halves[h] = halves[h] + jnp.where(from_half == h, got_z[e], 0.0)
    my_row = pos_y * 2 + pos_z
    lanes = iota((16, 128), 1)
    for h in range(2):
        line = jnp.sum(jnp.where(iota((8, 128), 0) == my_row, halves[h], 0.0), axis=0, keepdims=True)
        line = jnp.broadcast_to(line, (16, 128))
        band = 16 * part + iota((16, 128), 0)
        for side in range(2):
            one = jnp.where(lanes == band + side * BANDS, line, 0.0)
            out_ref[h, :, side : side + 1] = jnp.sum(one, axis=1, keepdims=True)

    for copy in list(copies.values()) + [far_copy] + x_copies + y_copies + z_copies:
        copy.wait_send()


def body(inverse_cov, channel_keep_mask, partner_ids, band_starts):
    vmem = pltpu.VMEM
    dma = pltpu.SemaphoreType.DMA
    return pl.pallas_call(
        body_kernel,
        out_shape=jax.ShapeDtypeStruct((2, 16, 2), F32),
        in_specs=[
            pl.BlockSpec(memory_space=pltpu.HBM),
            pl.BlockSpec(memory_space=pltpu.HBM),
            pl.BlockSpec(memory_space=pltpu.HBM),
            pl.BlockSpec(memory_space=pltpu.HBM),
        ],
        out_specs=pl.BlockSpec(memory_space=pltpu.VMEM),
        scratch_shapes=[
            vmem((1, 2 * PANEL), jnp.int32),
            vmem((1, 2), jnp.int32),
            vmem((2, BANDS), jnp.int32),
            vmem((PANEL, PANEL), F32),
            vmem((5, BLOCK, BLOCK), F32),
            vmem((REACH, 5, BLOCK, BLOCK), F32),
            vmem((REACH, 1, 2 * PANEL), jnp.int32),
            vmem((REACH, 1, 2), jnp.int32),
            vmem((REACH, 2, BLOCK, BLOCK), F32),
            vmem((2, BLOCK, BLOCK), F32),
            vmem((2, BLOCK, BLOCK), F32),
            vmem((BLOCK, PANEL), BF16),
            vmem((BLOCK, PANEL), BF16),
            vmem((PANEL, CLASSES * PANEL), BF16),
            vmem((PANEL, CLASSES * PANEL), BF16),
            vmem((PANEL, 2 * BANDS), BF16),
            vmem((PANEL, 2 * BANDS), BF16),
            vmem((CLASSES * PANEL, BANDS), BF16),
            vmem((PANEL, 2 * BANDS), BF16),
            vmem((PANEL, 2 * BANDS), BF16),
            vmem((2 * BANDS, PANEL), BF16),
            vmem((2 * BANDS, PANEL), BF16),
            vmem((2 * BANDS, PANEL), BF16),
            vmem((2 * BANDS, PANEL), BF16),
            vmem((CLASSES, BANDS, PANEL), BF16),
            vmem((PANEL, PANEL), BF16),
            vmem((PANEL, PANEL), BF16),
            vmem((CLASSES, ROWS, PANEL), F32),
            vmem((CLASSES, ROWS, 2 * BANDS), F32),
            vmem((2 * BANDS, PANEL), F32),
            vmem((2 * BANDS, 2 * BANDS), F32),
            vmem((BLOCK, CLASSES * PANEL), F32),
            vmem((2 * BANDS, CLASSES * PANEL), F32),
            vmem((BANDS, BANDS), F32),
            vmem((2 * BANDS, 2 * BANDS), F32),
            vmem((4, 8, 128), F32),
            vmem((3, 8, 128), F32),
            vmem((8, 128), F32),
            vmem((3, 8, 128), F32),
            vmem((8, 128), F32),
            vmem((7, 8, 128), F32),
            dma((REACH, 3)),
            dma((REACH, 3)),
            dma((2, REACH)),
            dma((2, REACH)),
            dma((2,)),
            dma((2,)),
            dma((9,)),
            dma((2, 3)),
            dma((2, 3)),
            dma((2, 7)),
        ],
        compiler_params=pltpu.CompilerParams(
            collective_id=0, has_side_effects=True, vmem_limit_bytes=67_043_328
        ),
    )(inverse_cov, channel_keep_mask, partner_ids, band_starts)


def solution(mesh):
    placed = (P("bl", "bp", None), P("bl", None), P("bl", None), P())
    return jax.shard_map(
        body, mesh=mesh, in_specs=placed, out_specs=P(None, "bp", "bl"), check_vma=False
    )
```

```python
import functools

import jax
import jax.numpy as jnp
from jax import lax
from jax.experimental import pallas as pl
from jax.experimental.pallas import tpu as pltpu
from jax.sharding import PartitionSpec as P

MESH = pl.DeviceIdType.MESH
F32 = jnp.float32
BF16 = jnp.bfloat16

GROUPS = 32
REACH = 4
SENDS = (-1, 2, -3, 4)
BLOCK = 128
TILE = 256
MESSAGES = ((0, 2, 0, 128), (2, 2, 0, 128), (4, 1, 0, 128))
STEPS = ((0, 0, 128), (1, 0, 128))
PANEL = 512
ROWS = 256
BANDS = 64
WINDOW = 128
CLASSES = 4
SCALE = 1.0 / (4 * GROUPS * WINDOW)


def split(x):
    hi = x.astype(BF16)
    return hi, (x - hi.astype(F32)).astype(BF16)


def mm(a, b):
    return jnp.dot(a, b, preferred_element_type=F32)


def dot3(a, b):
    rows = a[0].shape[0]
    both = mm(jnp.concatenate(a, axis=0), b[0])
    return both[:rows] + (mm(a[0], b[1]) + both[rows:])


def iota(shape, dim):
    return lax.broadcasted_iota(jnp.int32, shape, dim)


def down(row, count):
    return jnp.transpose(jnp.broadcast_to(row, (128, count)))


def body_kernel(
    inv_ref, mask_hbm, partner_hbm, start_hbm, out_ref,
    mask_ref, partner_ref, start_ref, own_raw, own_pack, got, got_mask, got_partner, row_marks,
    far_sum, got_far, turned_far, turned_corner, rows_hi, rows_lo,
    toep_hi, toep_lo, edge_hi, edge_lo, win, decay_hi, decay_lo,
    decay_t_hi, decay_t_lo, edge_t_hi, edge_t_lo, win_t, panel_hi, panel_lo, filt, filt_edge,
    outer, outer_decay, boxes, gram, total, mirror,
    sum_xy, got_xy, sum_z, got_z,
    send_sem, recv_sem, mask_sem, partner_sem, sib_sem, far_sem, own_sem, xy_sem, z_sem,
):
    me = lax.axis_index("bl")
    part = lax.axis_index("bp")
    half = part // 2
    core = part % 2
    pos_z = me // 16
    first = pl.multiple_of(core * ROWS, ROWS)
    col0 = pl.multiple_of(half * PANEL, PANEL)
    sibling = (me, part + 1 - 2 * core)

    def by_core(zero, one):
        return core * (one - zero) + zero

    def target(d):
        return ((me + GROUPS + SENDS[d]) % GROUPS, part)

    def source(d):
        return ((me + GROUPS - SENDS[d]) % GROUPS, part)

    near = [2 * core, 2 * core + 1]
    far = [by_core(2 + r, 1 - r) for r in range(2)]
    missing = [by_core(3 - r, r) for r in range(2)]
    missing_slot = [by_core(1 - r, r) for r in range(2)]
    pack = [(0, far[0]), (1, far[1]), (0, near[0]), (0, near[1]), (1, near[1])]

    def lanes_of(block):
        return pl.ds(pl.multiple_of(col0 + BLOCK * block, BLOCK), BLOCK)

    plane = me % 16

    def plane_peer(e):
        return (me - plane + (plane + e) % 16, part)

    spot = pos_z * 4 + part

    def z_peer(e):
        g = (spot + e) % 8
        return (me % 16 + 16 * (g // 4), g % 4)

    peers = (
        [target(d) for d in range(REACH)]
        + [source(d) for d in range(REACH)]
        + [plane_peer(e) for e in range(1, 16)]
        + [z_peer(e) for e in range(1, 8)]
    )
    barrier = pltpu.get_barrier_semaphore()
    for peer in peers:
        pl.semaphore_signal(barrier, inc=1, device_id=peer, device_id_type=MESH)

    locals_ = [
        pltpu.make_async_copy(
            inv_ref.at[0, BLOCK * r : BLOCK * (r + 1), lanes_of(c)], own_pack.at[p], own_sem.at[p]
        )
        for p, (r, c) in enumerate(pack)
    ]
    own_rows = own_raw.at[pl.ds(first, ROWS)]
    locals_.append(
        pltpu.make_async_copy(inv_ref.at[0, :, pl.ds(col0, PANEL)], own_rows, own_sem.at[5])
    )
    locals_.append(pltpu.make_async_copy(mask_hbm, mask_ref, own_sem.at[6]))
    locals_.append(pltpu.make_async_copy(partner_hbm, partner_ref, own_sem.at[7]))
    locals_.append(pltpu.make_async_copy(start_hbm, start_ref, own_sem.at[8]))
    for copy in locals_:
        copy.start()
    for copy in locals_:
        copy.wait()
    pl.semaphore_wait(barrier, len(peers))

    sib_copy = pltpu.make_async_remote_copy(
        src_ref=own_rows, dst_ref=own_rows,
        send_sem=sib_sem.at[0], recv_sem=sib_sem.at[1], device_id=sibling, device_id_type=MESH,
    )
    sib_copy.start()
    mask_copies = []
    for d in range(REACH):
        pairs = [(mask_ref, got_mask, mask_sem)]
        if SENDS[d] > 0:
            pairs.append((partner_ref, got_partner, partner_sem))
        for src, dst, sem in pairs:
            copy = pltpu.make_async_remote_copy(
                src_ref=src, dst_ref=dst.at[d], send_sem=sem.at[0, d], recv_sem=sem.at[1, d],
                device_id=target(d), device_id_type=MESH,
            )
            copy.start()
            mask_copies.append(copy)
    copies = {}
    for g, (p, count, row0, height) in enumerate(MESSAGES):
        for d in range(REACH):
            copy = pltpu.make_async_remote_copy(
                src_ref=own_pack.at[pl.ds(p, count), pl.ds(row0, height)],
                dst_ref=got.at[d, pl.ds(p, count), pl.ds(row0, height)],
                send_sem=send_sem.at[d, g], recv_sem=recv_sem.at[d, g],
                device_id=target(d), device_id_type=MESH,
            )
            copy.start()
            copies[d, g] = copy

    starts = start_ref[pl.ds(half, 1), :]
    starts2 = jnp.concatenate([starts, starts], axis=1)
    lane = iota((1, 2 * BANDS), 1)
    lane_class = lane % CLASSES
    rate = 1.0 / (1 + lane_class).astype(F32)
    is_left = lane < BANDS
    for r0 in range(0, PANEL, 128):
        pos = iota((128, 2 * BANDS), 0) + r0
        from_start = pos - starts2
        to_end = starts2 + (WINDOW - 1) - pos
        inside = (from_start >= 0) & (to_end >= 0)
        gap = jnp.where(is_left, -from_start, -to_end)
        edge = jnp.where(gap > 0, jnp.exp(-jnp.abs(gap).astype(F32) * rate), 0.0)
        edge_hi[r0 : r0 + 128, :], edge_lo[r0 : r0 + 128, :] = split(edge)
        decay = jnp.where(inside, jnp.exp(-jnp.abs(gap).astype(F32) * rate), 0.0)
        decay_hi[r0 : r0 + 128, :], decay_lo[r0 : r0 + 128, :] = split(decay)
        for l in range(CLASSES):
            one = jnp.where(inside & (lane_class == l), 1.0, 0.0)[:, :BANDS]
            win[l * PANEL + r0 : l * PANEL + r0 + 128, :] = one.astype(BF16)
    starts_t = down(starts2.astype(F32), 2 * BANDS).astype(jnp.int32)
    sub = iota((2 * BANDS, 128), 0)
    sub_class = sub % CLASSES
    rate_t = 1.0 / (1 + sub_class).astype(F32)
    is_left_t = sub < BANDS
    for r0 in range(0, PANEL, 128):
        pos = iota((2 * BANDS, 128), 1) + r0
        from_start = pos - starts_t
        to_end = starts_t + (WINDOW - 1) - pos
        inside = (from_start >= 0) & (to_end >= 0)
        gap = jnp.where(is_left_t, -from_start, -to_end)
        weight = jnp.exp(-jnp.abs(gap).astype(F32) * rate_t)
        edge_t_hi[:, r0 : r0 + 128], edge_t_lo[:, r0 : r0 + 128] = split(
            jnp.where(gap > 0, weight, 0.0)
        )
        decay_t_hi[:, r0 : r0 + 128], decay_t_lo[:, r0 : r0 + 128] = split(
            jnp.where(inside, weight, 0.0)
        )
        for l in range(CLASSES):
            one = jnp.where(inside & (sub_class == l), 1.0, 0.0)[:BANDS, :]
            win_t[l, :, r0 : r0 + 128] = one.astype(BF16)

    def fill(block, carry):
        r0 = pl.multiple_of(block * 128, 128)
        dist = jnp.abs(iota((128, PANEL), 0) + r0 - iota((128, PANEL), 1)).astype(F32)
        for l in range(CLASSES):
            hi, lo = split(jnp.exp(dist * (-1.0 / (1 + l))))
            toep_hi[pl.ds(r0, 128), l * PANEL : (l + 1) * PANEL] = hi
            toep_lo[pl.ds(r0, 128), l * PANEL : (l + 1) * PANEL] = lo
        return carry

    lax.fori_loop(0, PANEL // 128, fill, 0)

    sib_copy.wait()
    cols = mask_ref[:, pl.ds(col0, PANEL)].astype(F32)
    for r0 in range(0, PANEL, 128):
        marks = down(cols[:, r0 : r0 + 128], 128)
        for c0 in range(0, PANEL, 128):
            block = own_raw[r0 : r0 + 128, c0 : c0 + 128] * marks * cols[:, c0 : c0 + 128]
            panel_hi[r0 : r0 + 128, c0 : c0 + 128], panel_lo[r0 : r0 + 128, c0 : c0 + 128] = split(
                block
            )
    panel = (panel_hi[...], panel_lo[...])
    decays = (decay_hi[...], decay_lo[...])
    for l in range(CLASSES):
        rows = (
            toep_hi[pl.ds(first, ROWS), l * PANEL : (l + 1) * PANEL],
            toep_lo[pl.ds(first, ROWS), l * PANEL : (l + 1) * PANEL],
        )
        out = dot3(rows, panel)
        filt[l] = out
        filt_edge[l] = dot3(split(out), decays)
    outer[...] = dot3((edge_t_hi[...], edge_t_lo[...]), panel)
    outer_decay[...] = dot3(split(outer[...]), decays)

    for copy in mask_copies:
        copy.wait()
    total[...] = jnp.zeros_like(total)
    gram[...] = jnp.zeros_like(gram)
    boxes[...] = jnp.zeros_like(boxes)
    mirror[...] = jnp.zeros_like(mirror)
    for d in range(REACH):
        if SENDS[d] < 0:
            hits = jnp.where(partner_ref[...] == source(d)[0], 1.0, 0.0)
        else:
            hits = jnp.where(got_partner[d] == me, 1.0, 0.0)
        weight = hits[:, 0:1] + hits[:, 1:2]
        for r in range(2):
            marks = got_mask[d, :, lanes_of(near[r])].astype(F32) * weight
            row_marks[d, r] = down(marks, BLOCK)

    def summed(p, at=slice(0, BLOCK)):
        r, c = pack[p]
        out = 0.0
        for d in range(REACH):
            cols = got_mask[d, :, lanes_of(c)].astype(F32)
            out = out + got[d, p, at] * row_marks[d, r, at] * cols
        return out

    def put(block, value):
        hi, lo = split(value)
        spot = pl.ds(pl.multiple_of(BLOCK * block, BLOCK), BLOCK)
        rows_hi[: value.shape[0], spot] = hi
        rows_lo[: value.shape[0], spot] = lo

    far_copy = pltpu.make_async_remote_copy(
        src_ref=far_sum, dst_ref=got_far,
        send_sem=far_sem.at[0], recv_sem=far_sem.at[1], device_id=sibling, device_id_type=MESH,
    )
    for d in range(REACH):
        copies[d, 0].wait_recv()
    for r in range(2):
        far_sum[r] = summed(r)
    far_copy.start()
    for step, (k, row0, height) in enumerate(STEPS):
        y0 = k * BLOCK + row0
        at = slice(row0, row0 + height)
        for d in range(REACH):
            copies[d, step + 1].wait_recv()
        if step == 0:
            far_copy.wait_recv()
            for r in range(2):
                turned_far[r] = jnp.transpose(got_far[missing_slot[r]])
        put(far[k], far_sum[k, at])
        put(missing[k], turned_far[k, at])
        if k == 0:
            put(near[0], summed(2))
            corner = summed(3)
            put(near[1], corner)
            turned_corner[...] = jnp.transpose(corner)
        else:
            put(near[0], turned_corner[at])
            put(near[1], summed(4, at))
        rows = (rows_hi[:height], rows_lo[:height])
        here = pl.ds(pl.multiple_of(first + k * BLOCK, BLOCK), BLOCK)
        decay_t = (decay_t_hi[:, here], decay_t_lo[:, here])
        edges = dot3(rows, (edge_hi[...], edge_lo[...]))
        mirror[...] += dot3(decay_t, split(edges))
        rims = []
        for lb in range(CLASSES):
            rim = edges * filt_edge[lb, y0 : y0 + BLOCK, :]
            rims.append(rim[:, :BANDS] + rim[:, BANDS:])
        inside = jnp.concatenate([win_t[lb, :, here] for lb in range(CLASSES)], axis=1)
        hi, lo = split(jnp.concatenate(rims, axis=0))
        total[...] -= mm(inside, hi) + mm(inside, lo)
        for la in range(CLASSES):
            for c0 in range(0, PANEL, TILE):
                span = slice(la * PANEL + c0, la * PANEL + c0 + TILE)
                out = dot3(rows, (toep_hi[:, span], toep_lo[:, span]))
                gram[:, span] += dot3(decay_t, split(out))
                hi, lo = split(
                    jnp.concatenate(
                        [out * filt[lb, y0 : y0 + BLOCK, c0 : c0 + TILE] for lb in range(la, CLASSES)],
                        axis=0,
                    )
                )
                above = inside[:, la * BLOCK :]
                boxes[:, span] += mm(above, hi) + mm(above, lo)
    fisher = total[...]
    for la in range(CLASSES):
        span = slice(la * PANEL, (la + 1) * PANEL)
        left = gram[:BANDS, span] * outer[:BANDS, :]
        right = gram[BANDS:, span] * outer[BANDS:, :]
        hi, lo = split(boxes[:, span] - (left + right))
        fisher = fisher + (mm(hi, win[span, :]) + mm(lo, win[span, :]))
    four = mirror[...] * outer_decay[...]
    fisher = fisher + (four[:BANDS, :BANDS] + four[:BANDS, BANDS:])
    fisher = fisher + (four[BANDS:, :BANDS] + four[BANDS:, BANDS:])
    row_class = iota((BANDS, BANDS), 0) % CLASSES
    col_class = iota((BANDS, BANDS), 1) % CLASSES
    kept = jnp.where(col_class <= row_class, fisher * SCALE, 0.0)
    wide = jnp.concatenate([kept, jnp.zeros_like(kept)], axis=1)
    turned_over = jnp.transpose(jnp.concatenate([wide, jnp.zeros_like(wide)], axis=0))
    fisher = kept + jnp.where(col_class > row_class, turned_over[:BANDS, :BANDS], 0.0)

    row = iota((128, BANDS), 0)
    owner = (row % 8) * 16 + row // 8
    col = iota((128, BANDS), 1)
    parts3 = []
    rest = fisher
    for _ in range(3):
        piece = rest.astype(BF16)
        parts3.append(piece)
        rest = rest - piece.astype(F32)
    turned = []
    for side in range(2):
        pick = jnp.where(col == 2 * owner + side, 1.0, 0.0).astype(BF16)
        turned.append(mm(pick, parts3[0]) + mm(pick, parts3[1]) + mm(pick, parts3[2]))
    placed = jnp.concatenate(turned, axis=1)
    sum_xy[...] = placed.reshape(16, 8, 128)

    xy_copies = []
    for e in range(1, 16):
        copy = pltpu.make_async_remote_copy(
            src_ref=sum_xy.at[(plane + e) % 16], dst_ref=got_xy.at[e - 1],
            send_sem=xy_sem.at[0, e - 1], recv_sem=xy_sem.at[1, e - 1],
            device_id=plane_peer(e), device_id_type=MESH,
        )
        copy.start()
        xy_copies.append(copy)
    tile = sum_xy[plane]
    for e in range(15):
        xy_copies[e].wait_recv()
        tile = tile + got_xy[e]
    sum_z[...] = tile
    z_copies = []
    for e in range(1, 8):
        copy = pltpu.make_async_remote_copy(
            src_ref=sum_z, dst_ref=got_z.at[e - 1],
            send_sem=z_sem.at[0, e - 1], recv_sem=z_sem.at[1, e - 1],
            device_id=z_peer(e), device_id_type=MESH,
        )
        copy.start()
        z_copies.append(copy)
    halves = [jnp.where(half == h, tile, 0.0) for h in range(2)]
    for e in range(7):
        z_copies[e].wait_recv()
        from_half = ((spot + 7 - e) % 8 % 4) // 2
        for h in range(2):
            halves[h] = halves[h] + jnp.where(from_half == h, got_z[e], 0.0)
    lanes = iota((2, 16, 128), 2)
    band = 16 * part + iota((2, 16, 128), 1) + BANDS * iota((2, 16, 128), 0)
    for h in range(2):
        line = jnp.where(pos_z == 0, halves[h][0:1], halves[h][1:2])
        line = jnp.broadcast_to(line[None], (2, 16, 128))
        out_ref[h] = jnp.sum(jnp.where(lanes == band, line, 0.0), axis=2)

    for copy in list(copies.values()) + [far_copy] + xy_copies + z_copies:
        copy.wait_send()


def body(inverse_cov, channel_keep_mask, partner_ids, band_starts):
    vmem = pltpu.VMEM
    dma = pltpu.SemaphoreType.DMA
    out = pl.pallas_call(
        body_kernel,
        out_shape=jax.ShapeDtypeStruct((2, 2, 16), F32),
        in_specs=[
            pl.BlockSpec(memory_space=pltpu.HBM),
            pl.BlockSpec(memory_space=pltpu.HBM),
            pl.BlockSpec(memory_space=pltpu.HBM),
            pl.BlockSpec(memory_space=pltpu.HBM),
        ],
        out_specs=pl.BlockSpec(memory_space=pltpu.VMEM),
        scratch_shapes=[
            vmem((1, 2 * PANEL), jnp.int32),
            vmem((1, 2), jnp.int32),
            vmem((2, BANDS), jnp.int32),
            vmem((PANEL, PANEL), F32),
            vmem((5, BLOCK, BLOCK), F32),
            vmem((REACH, 5, BLOCK, BLOCK), F32),
            vmem((REACH, 1, 2 * PANEL), jnp.int32),
            vmem((REACH, 1, 2), jnp.int32),
            vmem((REACH, 2, BLOCK, BLOCK), F32),
            vmem((2, BLOCK, BLOCK), F32),
            vmem((2, BLOCK, BLOCK), F32),
            vmem((2, BLOCK, BLOCK), F32),
            vmem((BLOCK, BLOCK), F32),
            vmem((BLOCK, PANEL), BF16),
            vmem((BLOCK, PANEL), BF16),
            vmem((PANEL, CLASSES * PANEL), BF16),
            vmem((PANEL, CLASSES * PANEL), BF16),
            vmem((PANEL, 2 * BANDS), BF16),
            vmem((PANEL, 2 * BANDS), BF16),
            vmem((CLASSES * PANEL, BANDS), BF16),
            vmem((PANEL, 2 * BANDS), BF16),
            vmem((PANEL, 2 * BANDS), BF16),
            vmem((2 * BANDS, PANEL), BF16),
            vmem((2 * BANDS, PANEL), BF16),
            vmem((2 * BANDS, PANEL), BF16),
            vmem((2 * BANDS, PANEL), BF16),
            vmem((CLASSES, BANDS, PANEL), BF16),
            vmem((PANEL, PANEL), BF16),
            vmem((PANEL, PANEL), BF16),
            vmem((CLASSES, ROWS, PANEL), F32),
            vmem((CLASSES, ROWS, 2 * BANDS), F32),
            vmem((2 * BANDS, PANEL), F32),
            vmem((2 * BANDS, 2 * BANDS), F32),
            vmem((BANDS, CLASSES * PANEL), F32),
            vmem((2 * BANDS, CLASSES * PANEL), F32),
            vmem((BANDS, BANDS), F32),
            vmem((2 * BANDS, 2 * BANDS), F32),
            vmem((16, 8, 128), F32),
            vmem((15, 8, 128), F32),
            vmem((8, 128), F32),
            vmem((7, 8, 128), F32),
            dma((REACH, len(MESSAGES))),
            dma((REACH, len(MESSAGES))),
            dma((2, REACH)),
            dma((2, REACH)),
            dma((2,)),
            dma((2,)),
            dma((9,)),
            dma((2, 15)),
            dma((2, 7)),
        ],
        compiler_params=pltpu.CompilerParams(
            collective_id=0, has_side_effects=True, vmem_limit_bytes=67_043_328
        ),
    )(inverse_cov, channel_keep_mask, partner_ids, band_starts)
    return jnp.transpose(out, (0, 2, 1))


def solution(mesh):
    placed = (P("bl", "bp", None), P("bl", None), P("bl", None), P())
    return jax.shard_map(
        body, mesh=mesh, in_specs=placed, out_specs=P(None, "bp", "bl"), check_vma=False
    )
```

```python
import functools

import jax
import jax.numpy as jnp
from jax import lax
from jax.experimental import pallas as pl
from jax.experimental.pallas import tpu as pltpu
from jax.sharding import PartitionSpec as P

MESH = pl.DeviceIdType.MESH
F32 = jnp.float32
BF16 = jnp.bfloat16

GROUPS = 32
REACH = 4
SENDS = (-1, 2, -3, 4)
BLOCK = 128
TILE = 256
MESSAGES = ((0, 2), (2, 2), (4, 1))
PANEL = 512
ROWS = 256
BANDS = 64
WINDOW = 128
CLASSES = 4
SCALE = 1.0 / (4 * GROUPS * WINDOW)


def split(x):
    hi = x.astype(BF16)
    return hi, (x - hi.astype(F32)).astype(BF16)


def mm(a, b):
    return jnp.dot(a, b, preferred_element_type=F32)


def dot3(a, b):
    rows = a[0].shape[0]
    both = mm(jnp.concatenate(a, axis=0), b[0])
    return both[:rows] + (mm(a[0], b[1]) + both[rows:])


def iota(shape, dim):
    return lax.broadcasted_iota(jnp.int32, shape, dim)


def down(row, count):
    return jnp.transpose(jnp.broadcast_to(row, (128, count)))


def body_kernel(
    inv_ref, mask_hbm, partner_hbm, start_hbm, out_ref,
    mask_ref, partner_ref, start_ref, own_raw, own_pack, got, got_mask, got_partner, row_marks,
    far_sum, got_far, far_edges, far_out, turned_corner, rows_hi, rows_lo,
    toep_hi, toep_lo, edge_hi, edge_lo, win, decay_hi, decay_lo,
    decay_t_hi, decay_t_lo, edge_t_hi, edge_t_lo, win_t, panel_hi, panel_lo, filt, filt_edge,
    outer, outer_decay, boxes, gram, total, mirror,
    sum_xy, got_xy, sum_z, got_z,
    send_sem, recv_sem, mask_sem, partner_sem, sib_sem, far_sem, own_sem, xy_sem, z_sem,
):
    me = lax.axis_index("bl")
    part = lax.axis_index("bp")
    half = part // 2
    core = part % 2
    pos_z = me // 16
    first = pl.multiple_of(core * ROWS, ROWS)
    col0 = pl.multiple_of(half * PANEL, PANEL)
    sibling = (me, part + 1 - 2 * core)

    def by_core(zero, one):
        return core * (one - zero) + zero

    def target(d):
        return ((me + GROUPS + SENDS[d]) % GROUPS, part)

    def source(d):
        return ((me + GROUPS - SENDS[d]) % GROUPS, part)

    near = [2 * core, 2 * core + 1]
    far = [by_core(2 + r, 1 - r) for r in range(2)]
    missing = [by_core(3 - r, r) for r in range(2)]
    missing_slot = [by_core(1 - r, r) for r in range(2)]
    pack = [(0, far[0]), (1, far[1]), (0, near[0]), (0, near[1]), (1, near[1])]

    def lanes_of(block):
        return pl.ds(pl.multiple_of(col0 + BLOCK * block, BLOCK), BLOCK)

    plane = me % 16

    def plane_peer(e):
        return (me - plane + (plane + e) % 16, part)

    spot = pos_z * 4 + part

    def z_peer(e):
        g = (spot + e) % 8
        return (me % 16 + 16 * (g // 4), g % 4)

    peers = (
        [target(d) for d in range(REACH)]
        + [source(d) for d in range(REACH)]
        + [plane_peer(e) for e in range(1, 16)]
        + [z_peer(e) for e in range(1, 8)]
    )
    locals_ = [
        pltpu.make_async_copy(
            inv_ref.at[0, BLOCK * r : BLOCK * (r + 1), lanes_of(c)], own_pack.at[p], own_sem.at[p]
        )
        for p, (r, c) in enumerate(pack)
    ]
    own_rows = own_raw.at[pl.ds(first, ROWS)]
    locals_.append(
        pltpu.make_async_copy(inv_ref.at[0, :, pl.ds(col0, PANEL)], own_rows, own_sem.at[5])
    )
    locals_.append(pltpu.make_async_copy(mask_hbm, mask_ref, own_sem.at[6]))
    locals_.append(pltpu.make_async_copy(partner_hbm, partner_ref, own_sem.at[7]))
    locals_.append(pltpu.make_async_copy(start_hbm, start_ref, own_sem.at[8]))
    for copy in locals_:
        copy.start()
    barrier = pltpu.get_barrier_semaphore()
    for peer in peers:
        pl.semaphore_signal(barrier, inc=1, device_id=peer, device_id_type=MESH)

    for n in (0, 1, 6, 7):
        locals_[n].wait()
    pl.semaphore_wait(barrier, len(peers))

    mask_copies = []
    for d in range(REACH):
        pairs = [(mask_ref, got_mask, mask_sem)]
        if SENDS[d] > 0:
            pairs.append((partner_ref, got_partner, partner_sem))
        for src, dst, sem in pairs:
            copy = pltpu.make_async_remote_copy(
                src_ref=src, dst_ref=dst.at[d], send_sem=sem.at[0, d], recv_sem=sem.at[1, d],
                device_id=target(d), device_id_type=MESH,
            )
            copy.start()
            mask_copies.append(copy)
    copies = {}
    for g, (p, count) in enumerate(MESSAGES):
        if g:
            for n in range(p, p + count):
                locals_[n].wait()
        for d in range(REACH):
            copy = pltpu.make_async_remote_copy(
                src_ref=own_pack.at[pl.ds(p, count)],
                dst_ref=got.at[d, pl.ds(p, count)],
                send_sem=send_sem.at[d, g], recv_sem=recv_sem.at[d, g],
                device_id=target(d), device_id_type=MESH,
            )
            copy.start()
            copies[d, g] = copy
    locals_[5].wait()
    sib_copy = pltpu.make_async_remote_copy(
        src_ref=own_rows, dst_ref=own_rows,
        send_sem=sib_sem.at[0], recv_sem=sib_sem.at[1], device_id=sibling, device_id_type=MESH,
    )
    sib_copy.start()

    locals_[8].wait()
    starts = start_ref[pl.ds(half, 1), :]
    starts2 = jnp.concatenate([starts, starts], axis=1)
    lane = iota((1, 2 * BANDS), 1)
    lane_class = lane % CLASSES
    rate = 1.0 / (1 + lane_class).astype(F32)
    is_left = lane < BANDS
    for r0 in range(0, PANEL, 128):
        pos = iota((128, 2 * BANDS), 0) + r0
        from_start = pos - starts2
        to_end = starts2 + (WINDOW - 1) - pos
        inside = (from_start >= 0) & (to_end >= 0)
        gap = jnp.where(is_left, -from_start, -to_end)
        edge = jnp.where(gap > 0, jnp.exp(-jnp.abs(gap).astype(F32) * rate), 0.0)
        edge_hi[r0 : r0 + 128, : 2 * BANDS], edge_lo[r0 : r0 + 128, : 2 * BANDS] = split(edge)
        side_lane = iota((128, 2 * BANDS), 1)
        low_half = (side_lane + core) % 2 == 1
        reach = jnp.where(low_half, TILE - 1 - pos, pos - TILE)
        side_rate = 1.0 / (1 + (side_lane // 2) % CLASSES).astype(F32)
        spill = jnp.where(
            (reach >= 0) & (side_lane < 2 * CLASSES), jnp.exp(-jnp.abs(reach).astype(F32) * side_rate), 0.0
        )
        edge_hi[r0 : r0 + 128, 2 * BANDS :], edge_lo[r0 : r0 + 128, 2 * BANDS :] = split(spill)
        decay = jnp.where(inside, jnp.exp(-jnp.abs(gap).astype(F32) * rate), 0.0)
        decay_hi[r0 : r0 + 128, :], decay_lo[r0 : r0 + 128, :] = split(decay)
        for l in range(CLASSES):
            one = jnp.where(inside & (lane_class == l), 1.0, 0.0)[:, :BANDS]
            win[l * PANEL + r0 : l * PANEL + r0 + 128, :] = one.astype(BF16)
    starts_t = down(starts2.astype(F32), 2 * BANDS).astype(jnp.int32)
    sub = iota((2 * BANDS, 128), 0)
    sub_class = sub % CLASSES
    rate_t = 1.0 / (1 + sub_class).astype(F32)
    is_left_t = sub < BANDS
    for r0 in range(0, PANEL, 128):
        pos = iota((2 * BANDS, 128), 1) + r0
        from_start = pos - starts_t
        to_end = starts_t + (WINDOW - 1) - pos
        inside = (from_start >= 0) & (to_end >= 0)
        gap = jnp.where(is_left_t, -from_start, -to_end)
        weight = jnp.exp(-jnp.abs(gap).astype(F32) * rate_t)
        edge_t_hi[:, r0 : r0 + 128], edge_t_lo[:, r0 : r0 + 128] = split(
            jnp.where(gap > 0, weight, 0.0)
        )
        decay_t_hi[:, r0 : r0 + 128], decay_t_lo[:, r0 : r0 + 128] = split(
            jnp.where(inside, weight, 0.0)
        )
        for l in range(CLASSES):
            one = jnp.where(inside & (sub_class == l), 1.0, 0.0)[:BANDS, :]
            win_t[l, :, r0 : r0 + 128] = one.astype(BF16)

    def fill(block, carry):
        r0 = pl.multiple_of(block * 128, 128)
        dist = jnp.abs(iota((128, PANEL), 0) + r0 - iota((128, PANEL), 1)).astype(F32)
        for l in range(CLASSES):
            hi, lo = split(jnp.exp(dist * (-1.0 / (1 + l))))
            toep_hi[pl.ds(r0, 128), l * PANEL : (l + 1) * PANEL] = hi
            toep_lo[pl.ds(r0, 128), l * PANEL : (l + 1) * PANEL] = lo
        return carry

    lax.fori_loop(0, PANEL // 128, fill, 0)

    sib_copy.wait()
    cols = mask_ref[:, pl.ds(col0, PANEL)].astype(F32)
    for r0 in range(0, PANEL, 128):
        marks = down(cols[:, r0 : r0 + 128], 128)
        for c0 in range(0, PANEL, 128):
            block = own_raw[r0 : r0 + 128, c0 : c0 + 128] * marks * cols[:, c0 : c0 + 128]
            panel_hi[r0 : r0 + 128, c0 : c0 + 128], panel_lo[r0 : r0 + 128, c0 : c0 + 128] = split(
                block
            )
    panel = (panel_hi[...], panel_lo[...])
    decays = (decay_hi[...], decay_lo[...])
    for l in range(CLASSES):
        rows = (
            toep_hi[pl.ds(first, ROWS), l * PANEL : (l + 1) * PANEL],
            toep_lo[pl.ds(first, ROWS), l * PANEL : (l + 1) * PANEL],
        )
        out = dot3(rows, panel)
        filt[l] = out
        filt_edge[l] = dot3(split(out), decays)
    outer[...] = dot3((edge_t_hi[...], edge_t_lo[...]), panel)
    outer_decay[...] = dot3(split(outer[...]), decays)

    for copy in mask_copies:
        copy.wait()
    total[...] = jnp.zeros_like(total)
    boxes[...] = jnp.zeros_like(boxes)
    gram[...] = jnp.zeros_like(gram)
    mirror[...] = jnp.zeros_like(mirror)
    for d in range(REACH):
        if SENDS[d] < 0:
            hits = jnp.where(partner_ref[...] == source(d)[0], 1.0, 0.0)
        else:
            hits = jnp.where(got_partner[d] == me, 1.0, 0.0)
        weight = hits[:, 0:1] + hits[:, 1:2]
        for r in range(2):
            marks = got_mask[d, :, lanes_of(near[r])].astype(F32) * weight
            row_marks[d, r] = down(marks, BLOCK)

    def summed(p):
        r, c = pack[p]
        out = 0.0
        for d in range(REACH):
            cols = got_mask[d, :, lanes_of(c)].astype(F32)
            out = out + got[d, p] * row_marks[d, r] * cols
        return out

    def filtered(rows, l):
        square = slice(l * PANEL, l * PANEL + TILE)
        return dot3(rows, (toep_hi[:TILE, square], toep_lo[:TILE, square]))

    near_half = pl.ds(first, TILE)
    far_half = pl.ds(pl.multiple_of(TILE - first, TILE), TILE)

    far_copy = pltpu.make_async_remote_copy(
        src_ref=far_sum, dst_ref=got_far,
        send_sem=far_sem.at[0], recv_sem=far_sem.at[1], device_id=sibling, device_id_type=MESH,
    )
    for d in range(REACH):
        copies[d, 0].wait_recv()
    for r in range(2):
        far_sum[r] = summed(r)
    far_copy.start()
    far_copy.wait_recv()
    far_block = 2 - 2 * core
    for r in range(2):
        for block, value in (
            (far[r], far_sum[r]), (missing[r], jnp.transpose(got_far[missing_slot[r]]))
        ):
            lanes_at = pl.ds(pl.multiple_of(BLOCK * (block - far_block), BLOCK), BLOCK)
            hi, lo = split(value)
            rows_hi[r * BLOCK : (r + 1) * BLOCK, lanes_at] = hi
            rows_lo[r * BLOCK : (r + 1) * BLOCK, lanes_at] = lo
    rows = (rows_hi[...], rows_lo[...])
    far_edges[...] = dot3(rows, (edge_hi[far_half, :], edge_lo[far_half, :]))
    far_gram = dot3((decay_t_hi[:, near_half], decay_t_lo[:, near_half]), rows)
    gram_hi, gram_lo = split(far_gram)
    stack = tuple(jnp.concatenate(pair, axis=0) for pair in ((rows[0], gram_hi), (rows[1], gram_lo)))
    for l in range(CLASSES):
        far_out[:, l * TILE : (l + 1) * TILE] = filtered(stack, l)

    in_low = core == 0
    tile_lane = iota((1, TILE), 1).astype(F32)
    rises = []
    for l in range(CLASSES):
        to_low = jnp.exp((tile_lane - TILE) * (1.0 / (1 + l)))
        to_high = jnp.exp((tile_lane + 1.0) * (-1.0 / (1 + l)))
        rises.append((jnp.where(in_low, to_low, to_high), jnp.where(in_low, to_high, to_low)))
    for k in range(2):
        y0 = k * BLOCK
        for d in range(REACH):
            copies[d, k + 1].wait_recv()
        if k == 0:
            corner = summed(3)
            blocks = (summed(2), corner)
            turned_corner[...] = jnp.transpose(corner)
        else:
            blocks = (turned_corner[...], summed(4))
        rows = split(jnp.concatenate(blocks, axis=1))
        here = pl.ds(pl.multiple_of(first + y0, BLOCK), BLOCK)
        decay_t = (decay_t_hi[:, here], decay_t_lo[:, here])
        edges = far_edges[y0 : y0 + BLOCK, :] + dot3(rows, (edge_hi[near_half, :], edge_lo[near_half, :]))
        mirror[...] += dot3(decay_t, split(edges))
        gram[...] += dot3(decay_t, rows)
        stack = rows
        if k == 1:
            near_gram = split(gram[...])
            stack = tuple(jnp.concatenate((a, b), axis=0) for a, b in zip(rows, near_gram))
        rims = []
        for lb in range(CLASSES):
            rim = edges[:, : 2 * BANDS] * filt_edge[lb, y0 : y0 + BLOCK, :]
            rims.append(rim[:, :BANDS] + rim[:, BANDS:])
        inside = jnp.concatenate([win_t[lb, :, here] for lb in range(CLASSES)], axis=1)
        hi, lo = split(jnp.concatenate(rims, axis=0))
        total[...] -= mm(inside, hi) + mm(inside, lo)
        for la in range(CLASSES):
            near_out = filtered(stack, la)
            above = inside[:, la * BLOCK :]
            tile = slice(la * TILE, (la + 1) * TILE)
            for j, half_cols in enumerate((near_half, far_half)):
                lane_col = 2 * BANDS + 2 * la + j

                def square(own, far_rows, source):
                    plain = near_out[own : own + BLOCK] if j == 0 else far_out[far_rows, tile]
                    return plain + source[:, lane_col : lane_col + 1] * rises[la][j]

                out = square(0, slice(y0, y0 + BLOCK), edges)
                hi, lo = split(
                    jnp.concatenate(
                        [out * filt[lb, y0 : y0 + BLOCK, half_cols] for lb in range(la, CLASSES)],
                        axis=0,
                    )
                )
                box = mm(above, hi) + mm(above, lo)
                if k == 1:
                    rim = square(BLOCK, slice(2 * BLOCK, 3 * BLOCK), mirror[...]) * outer[:, half_cols]
                    box = box - (rim[:BANDS] + rim[BANDS:])
                span = slice(la * PANEL + j * TILE, la * PANEL + (j + 1) * TILE)
                boxes[:, span] += box
    fisher = total[...]
    for la in range(CLASSES):
        for j, half_first in enumerate((first, TILE - first)):
            hi, lo = split(boxes[:, la * PANEL + j * TILE : la * PANEL + (j + 1) * TILE])
            channels = win[pl.ds(pl.multiple_of(la * PANEL + half_first, TILE), TILE), :]
            fisher = fisher + (mm(hi, channels) + mm(lo, channels))
    four = mirror[:, : 2 * BANDS] * outer_decay[...]
    fisher = fisher + (four[:BANDS, :BANDS] + four[:BANDS, BANDS:])
    fisher = fisher + (four[BANDS:, :BANDS] + four[BANDS:, BANDS:])
    row_class = iota((BANDS, BANDS), 0) % CLASSES
    col_class = iota((BANDS, BANDS), 1) % CLASSES
    kept = jnp.where(col_class <= row_class, fisher * SCALE, 0.0)
    wide = jnp.concatenate([kept, jnp.zeros_like(kept)], axis=1)
    turned_over = jnp.transpose(jnp.concatenate([wide, jnp.zeros_like(wide)], axis=0))
    fisher = kept + jnp.where(col_class > row_class, turned_over[:BANDS, :BANDS], 0.0)

    row = iota((128, BANDS), 0)
    owner = (row % 8) * 16 + row // 8
    col = iota((128, BANDS), 1)
    parts3 = []
    rest = fisher
    for _ in range(3):
        piece = rest.astype(BF16)
        parts3.append(piece)
        rest = rest - piece.astype(F32)
    turned = []
    for side in range(2):
        pick = jnp.where(col == 2 * owner + side, 1.0, 0.0).astype(BF16)
        turned.append(mm(pick, parts3[0]) + mm(pick, parts3[1]) + mm(pick, parts3[2]))
    placed = jnp.concatenate(turned, axis=1)
    sum_xy[...] = placed.reshape(16, 8, 128)

    xy_copies = []
    for e in range(1, 16):
        copy = pltpu.make_async_remote_copy(
            src_ref=sum_xy.at[(plane + e) % 16], dst_ref=got_xy.at[e - 1],
            send_sem=xy_sem.at[0, e - 1], recv_sem=xy_sem.at[1, e - 1],
            device_id=plane_peer(e), device_id_type=MESH,
        )
        copy.start()
        xy_copies.append(copy)
    tile = sum_xy[plane]
    for e in range(15):
        xy_copies[e].wait_recv()
        tile = tile + got_xy[e]
    sum_z[...] = tile
    z_copies = []
    for e in range(1, 8):
        copy = pltpu.make_async_remote_copy(
            src_ref=sum_z, dst_ref=got_z.at[e - 1],
            send_sem=z_sem.at[0, e - 1], recv_sem=z_sem.at[1, e - 1],
            device_id=z_peer(e), device_id_type=MESH,
        )
        copy.start()
        z_copies.append(copy)
    halves = [jnp.where(half == h, tile, 0.0) for h in range(2)]
    for e in range(7):
        z_copies[e].wait_recv()
        from_half = ((spot + 7 - e) % 8 % 4) // 2
        for h in range(2):
            halves[h] = halves[h] + jnp.where(from_half == h, got_z[e], 0.0)
    lanes = iota((2, 16, 128), 2)
    band = 16 * part + iota((2, 16, 128), 1) + BANDS * iota((2, 16, 128), 0)
    for h in range(2):
        line = jnp.where(pos_z == 0, halves[h][0:1], halves[h][1:2])
        line = jnp.broadcast_to(line[None], (2, 16, 128))
        out_ref[h] = jnp.sum(jnp.where(lanes == band, line, 0.0), axis=2)

    for copy in list(copies.values()) + [far_copy] + xy_copies + z_copies:
        copy.wait_send()


def body(inverse_cov, channel_keep_mask, partner_ids, band_starts):
    vmem = pltpu.VMEM
    dma = pltpu.SemaphoreType.DMA
    out = pl.pallas_call(
        body_kernel,
        out_shape=jax.ShapeDtypeStruct((2, 2, 16), F32),
        in_specs=[
            pl.BlockSpec(memory_space=pltpu.HBM),
            pl.BlockSpec(memory_space=pltpu.HBM),
            pl.BlockSpec(memory_space=pltpu.HBM),
            pl.BlockSpec(memory_space=pltpu.HBM),
        ],
        out_specs=pl.BlockSpec(memory_space=pltpu.VMEM),
        scratch_shapes=[
            vmem((1, 2 * PANEL), jnp.int32),
            vmem((1, 2), jnp.int32),
            vmem((2, BANDS), jnp.int32),
            vmem((PANEL, PANEL), F32),
            vmem((5, BLOCK, BLOCK), F32),
            vmem((REACH, 5, BLOCK, BLOCK), F32),
            vmem((REACH, 1, 2 * PANEL), jnp.int32),
            vmem((REACH, 1, 2), jnp.int32),
            vmem((REACH, 2, BLOCK, BLOCK), F32),
            vmem((2, BLOCK, BLOCK), F32),
            vmem((2, BLOCK, BLOCK), F32),
            vmem((ROWS, 4 * BANDS), F32),
            vmem((ROWS + 2 * BANDS, CLASSES * TILE), F32),
            vmem((BLOCK, BLOCK), F32),
            vmem((ROWS, TILE), BF16),
            vmem((ROWS, TILE), BF16),
            vmem((PANEL, CLASSES * PANEL), BF16),
            vmem((PANEL, CLASSES * PANEL), BF16),
            vmem((PANEL, 4 * BANDS), BF16),
            vmem((PANEL, 4 * BANDS), BF16),
            vmem((CLASSES * PANEL, BANDS), BF16),
            vmem((PANEL, 2 * BANDS), BF16),
            vmem((PANEL, 2 * BANDS), BF16),
            vmem((2 * BANDS, PANEL), BF16),
            vmem((2 * BANDS, PANEL), BF16),
            vmem((2 * BANDS, PANEL), BF16),
            vmem((2 * BANDS, PANEL), BF16),
            vmem((CLASSES, BANDS, PANEL), BF16),
            vmem((PANEL, PANEL), BF16),
            vmem((PANEL, PANEL), BF16),
            vmem((CLASSES, ROWS, PANEL), F32),
            vmem((CLASSES, ROWS, 2 * BANDS), F32),
            vmem((2 * BANDS, PANEL), F32),
            vmem((2 * BANDS, 2 * BANDS), F32),
            vmem((BANDS, CLASSES * PANEL), F32),
            vmem((2 * BANDS, TILE), F32),
            vmem((BANDS, BANDS), F32),
            vmem((2 * BANDS, 4 * BANDS), F32),
            vmem((16, 8, 128), F32),
            vmem((15, 8, 128), F32),
            vmem((8, 128), F32),
            vmem((7, 8, 128), F32),
            dma((REACH, len(MESSAGES))),
            dma((REACH, len(MESSAGES))),
            dma((2, REACH)),
            dma((2, REACH)),
            dma((2,)),
            dma((2,)),
            dma((9,)),
            dma((2, 15)),
            dma((2, 7)),
        ],
        compiler_params=pltpu.CompilerParams(
            collective_id=0, has_side_effects=True, vmem_limit_bytes=67_043_328
        ),
    )(inverse_cov, channel_keep_mask, partner_ids, band_starts)
    return jnp.transpose(out, (0, 2, 1))


def solution(mesh):
    placed = (P("bl", "bp", None), P("bl", None), P("bl", None), P())
    return jax.shard_map(
        body, mesh=mesh, in_specs=placed, out_specs=P(None, "bp", "bl"), check_vma=False
    )
```

```python
import functools

import jax
import jax.numpy as jnp
from jax import lax
from jax.experimental import pallas as pl
from jax.experimental.pallas import tpu as pltpu
from jax.sharding import PartitionSpec as P

MESH = pl.DeviceIdType.MESH
F32 = jnp.float32
BF16 = jnp.bfloat16

GROUPS = 32
REACH = 4
SENDS = (-1, 2, -3, 4)
BLOCK = 128
TILE = 256
MESSAGES = ((0, 2), (2, 2), (4, 1))
PANEL = 512
ROWS = 256
BANDS = 64
WINDOW = 128
CLASSES = 4
SCALE = 1.0 / (4 * GROUPS * WINDOW)


def split(x):
    hi = x.astype(BF16)
    return hi, (x - hi.astype(F32)).astype(BF16)


def mm(a, b):
    return jnp.dot(a, b, preferred_element_type=F32)


def dot3(a, b):
    rows = a[0].shape[0]
    both = mm(jnp.concatenate(a, axis=0), b[0])
    return both[:rows] + (mm(a[0], b[1]) + both[rows:])


def iota(shape, dim):
    return lax.broadcasted_iota(jnp.int32, shape, dim)


def down(row, count):
    return jnp.transpose(jnp.broadcast_to(row, (128, count)))


def body_kernel(
    inv_ref, mask_hbm, partner_hbm, start_hbm, out_ref,
    mask_ref, partner_ref, start_ref, own_raw, own_pack, got, got_mask, got_partner, row_marks,
    far_sum, got_far, far_edges, far_out, turned_corner, rows_hi, rows_lo,
    toep_hi, toep_lo, edge_hi, edge_lo, win, decay_hi, decay_lo,
    decay_t_hi, decay_t_lo, edge_t_hi, edge_t_lo, win_t, panel_hi, panel_lo, filt, filt_edge,
    outer, outer_decay, boxes, gram, total, mirror,
    sum_xy, got_xy, sum_z, got_z,
    send_sem, recv_sem, mask_sem, partner_sem, sib_sem, far_sem, own_sem, xy_sem, z_sem,
):
    me = lax.axis_index("bl")
    part = lax.axis_index("bp")
    half = part // 2
    core = part % 2
    pos_z = me // 16
    first = pl.multiple_of(core * ROWS, ROWS)
    col0 = pl.multiple_of(half * PANEL, PANEL)
    sibling = (me, part + 1 - 2 * core)

    def by_core(zero, one):
        return core * (one - zero) + zero

    def target(d):
        return ((me + GROUPS + SENDS[d]) % GROUPS, part)

    def source(d):
        return ((me + GROUPS - SENDS[d]) % GROUPS, part)

    near = [2 * core, 2 * core + 1]
    far = [by_core(2 + r, 1 - r) for r in range(2)]
    missing = [by_core(3 - r, r) for r in range(2)]
    missing_slot = [by_core(1 - r, r) for r in range(2)]
    pack = [(0, far[0]), (1, far[1]), (0, near[0]), (0, near[1]), (1, near[1])]

    def lanes_of(block):
        return pl.ds(pl.multiple_of(col0 + BLOCK * block, BLOCK), BLOCK)

    plane = me % 16

    def plane_peer(e):
        return (me - plane + (plane + e) % 16, part)

    spot = pos_z * 4 + part

    def z_peer(e):
        g = (spot + e) % 8
        return (me % 16 + 16 * (g // 4), g % 4)

    peers = (
        [target(d) for d in range(REACH)]
        + [source(d) for d in range(REACH)]
        + [plane_peer(e) for e in range(1, 16)]
        + [z_peer(e) for e in range(1, 8)]
    )
    barrier = pltpu.get_barrier_semaphore()
    for peer in peers[: 2 * REACH]:
        pl.semaphore_signal(barrier, inc=1, device_id=peer, device_id_type=MESH)
    locals_ = [
        pltpu.make_async_copy(
            inv_ref.at[0, BLOCK * r : BLOCK * (r + 1), lanes_of(c)], own_pack.at[p], own_sem.at[p]
        )
        for p, (r, c) in enumerate(pack)
    ]
    own_rows = own_raw.at[pl.ds(first, ROWS)]
    locals_.append(
        pltpu.make_async_copy(inv_ref.at[0, :, pl.ds(col0, PANEL)], own_rows, own_sem.at[5])
    )
    locals_.append(pltpu.make_async_copy(mask_hbm, mask_ref, own_sem.at[6]))
    locals_.append(pltpu.make_async_copy(partner_hbm, partner_ref, own_sem.at[7]))
    locals_.append(pltpu.make_async_copy(start_hbm, start_ref, own_sem.at[8]))
    for copy in locals_:
        copy.start()
    for peer in peers[2 * REACH :]:
        pl.semaphore_signal(barrier, inc=1, device_id=peer, device_id_type=MESH)
    for n in (0, 1, 6, 7):
        locals_[n].wait()
    pl.semaphore_wait(barrier, len(peers))

    mask_copies = []
    for d in range(REACH):
        pairs = [(mask_ref, got_mask, mask_sem)]
        if SENDS[d] > 0:
            pairs.append((partner_ref, got_partner, partner_sem))
        for src, dst, sem in pairs:
            copy = pltpu.make_async_remote_copy(
                src_ref=src, dst_ref=dst.at[d], send_sem=sem.at[0, d], recv_sem=sem.at[1, d],
                device_id=target(d), device_id_type=MESH,
            )
            copy.start()
            mask_copies.append(copy)
    copies = {}
    for g, (p, count) in enumerate(MESSAGES):
        if g:
            for n in range(p, p + count):
                locals_[n].wait()
        for d in range(REACH):
            copy = pltpu.make_async_remote_copy(
                src_ref=own_pack.at[pl.ds(p, count)],
                dst_ref=got.at[d, pl.ds(p, count)],
                send_sem=send_sem.at[d, g], recv_sem=recv_sem.at[d, g],
                device_id=target(d), device_id_type=MESH,
            )
            copy.start()
            copies[d, g] = copy
    locals_[5].wait()
    sib_copy = pltpu.make_async_remote_copy(
        src_ref=own_rows, dst_ref=own_rows,
        send_sem=sib_sem.at[0], recv_sem=sib_sem.at[1], device_id=sibling, device_id_type=MESH,
    )
    sib_copy.start()

    locals_[8].wait()
    starts = start_ref[pl.ds(half, 1), :]
    starts2 = jnp.concatenate([starts, starts], axis=1)
    lane = iota((1, 2 * BANDS), 1)
    lane_class = lane % CLASSES
    rate = 1.0 / (1 + lane_class).astype(F32)
    is_left = lane < BANDS
    for r0 in range(0, PANEL, 128):
        pos = iota((128, 2 * BANDS), 0) + r0
        from_start = pos - starts2
        to_end = starts2 + (WINDOW - 1) - pos
        inside = (from_start >= 0) & (to_end >= 0)
        gap = jnp.where(is_left, -from_start, -to_end)
        edge = jnp.where(gap > 0, jnp.exp(-jnp.abs(gap).astype(F32) * rate), 0.0)
        edge_hi[r0 : r0 + 128, : 2 * BANDS], edge_lo[r0 : r0 + 128, : 2 * BANDS] = split(edge)
        side_lane = iota((128, 2 * BANDS), 1)
        low_half = (side_lane + core) % 2 == 1
        reach = jnp.where(low_half, TILE - 1 - pos, pos - TILE)
        side_rate = 1.0 / (1 + (side_lane // 2) % CLASSES).astype(F32)
        spill = jnp.where(
            (reach >= 0) & (side_lane < 2 * CLASSES), jnp.exp(-jnp.abs(reach).astype(F32) * side_rate), 0.0
        )
        edge_hi[r0 : r0 + 128, 2 * BANDS :], edge_lo[r0 : r0 + 128, 2 * BANDS :] = split(spill)
        decay = jnp.where(inside, jnp.exp(-jnp.abs(gap).astype(F32) * rate), 0.0)
        decay_hi[r0 : r0 + 128, :], decay_lo[r0 : r0 + 128, :] = split(decay)
        for l in range(CLASSES):
            one = jnp.where(inside & (lane_class == l), 1.0, 0.0)[:, :BANDS]
            win[l * PANEL + r0 : l * PANEL + r0 + 128, :] = one.astype(BF16)
    starts_t = down(starts2.astype(F32), 2 * BANDS).astype(jnp.int32)
    sub = iota((2 * BANDS, 128), 0)
    sub_class = sub % CLASSES
    rate_t = 1.0 / (1 + sub_class).astype(F32)
    is_left_t = sub < BANDS
    for r0 in range(0, PANEL, 128):
        pos = iota((2 * BANDS, 128), 1) + r0
        from_start = pos - starts_t
        to_end = starts_t + (WINDOW - 1) - pos
        inside = (from_start >= 0) & (to_end >= 0)
        gap = jnp.where(is_left_t, -from_start, -to_end)
        weight = jnp.exp(-jnp.abs(gap).astype(F32) * rate_t)
        edge_t_hi[:, r0 : r0 + 128], edge_t_lo[:, r0 : r0 + 128] = split(
            jnp.where(gap > 0, weight, 0.0)
        )
        decay_t_hi[:, r0 : r0 + 128], decay_t_lo[:, r0 : r0 + 128] = split(
            jnp.where(inside, weight, 0.0)
        )
        for l in range(CLASSES):
            one = jnp.where(inside & (sub_class == l), 1.0, 0.0)[:BANDS, :]
            win_t[l, :, r0 : r0 + 128] = one.astype(BF16)

    def fill(block, carry):
        r0 = pl.multiple_of(block * 128, 128)
        dist = jnp.abs(iota((128, PANEL), 0) + r0 - iota((128, PANEL), 1)).astype(F32)
        for l in range(CLASSES):
            hi, lo = split(jnp.exp(dist * (-1.0 / (1 + l))))
            toep_hi[pl.ds(r0, 128), l * PANEL : (l + 1) * PANEL] = hi
            toep_lo[pl.ds(r0, 128), l * PANEL : (l + 1) * PANEL] = lo
        return carry

    lax.fori_loop(0, PANEL // 128, fill, 0)

    sib_copy.wait()
    cols = mask_ref[:, pl.ds(col0, PANEL)].astype(F32)
    for r0 in range(0, PANEL, 128):
        marks = down(cols[:, r0 : r0 + 128], 128)
        for c0 in range(0, PANEL, 128):
            block = own_raw[r0 : r0 + 128, c0 : c0 + 128] * marks * cols[:, c0 : c0 + 128]
            panel_hi[r0 : r0 + 128, c0 : c0 + 128], panel_lo[r0 : r0 + 128, c0 : c0 + 128] = split(
                block
            )
    panel = (panel_hi[...], panel_lo[...])
    decays = (decay_hi[...], decay_lo[...])
    for l in range(CLASSES):
        rows = (
            toep_hi[pl.ds(first, ROWS), l * PANEL : (l + 1) * PANEL],
            toep_lo[pl.ds(first, ROWS), l * PANEL : (l + 1) * PANEL],
        )
        out = dot3(rows, panel)
        filt[l] = out
        filt_edge[l] = dot3(split(out), decays)
    outer[...] = dot3((edge_t_hi[...], edge_t_lo[...]), panel)
    outer_decay[...] = dot3(split(outer[...]), decays)

    for copy in mask_copies:
        copy.wait()
    total[...] = jnp.zeros_like(total)
    boxes[...] = jnp.zeros_like(boxes)
    gram[...] = jnp.zeros_like(gram)
    mirror[...] = jnp.zeros_like(mirror)
    for d in range(REACH):
        if SENDS[d] < 0:
            hits = jnp.where(partner_ref[...] == source(d)[0], 1.0, 0.0)
        else:
            hits = jnp.where(got_partner[d] == me, 1.0, 0.0)
        weight = hits[:, 0:1] + hits[:, 1:2]
        for r in range(2):
            marks = got_mask[d, :, lanes_of(near[r])].astype(F32) * weight
            row_marks[d, r] = down(marks, BLOCK)

    def summed(p):
        r, c = pack[p]
        out = 0.0
        for d in range(REACH):
            cols = got_mask[d, :, lanes_of(c)].astype(F32)
            out = out + got[d, p] * row_marks[d, r] * cols
        return out

    def filtered(rows, l):
        square = slice(l * PANEL, l * PANEL + TILE)
        return dot3(rows, (toep_hi[:TILE, square], toep_lo[:TILE, square]))

    near_half = pl.ds(first, TILE)
    far_half = pl.ds(pl.multiple_of(TILE - first, TILE), TILE)

    far_copy = pltpu.make_async_remote_copy(
        src_ref=far_sum, dst_ref=got_far,
        send_sem=far_sem.at[0], recv_sem=far_sem.at[1], device_id=sibling, device_id_type=MESH,
    )
    for d in range(REACH):
        copies[d, 0].wait_recv()
    for r in range(2):
        far_sum[r] = summed(r)
    far_copy.start()
    far_copy.wait_recv()
    far_block = 2 - 2 * core
    for r in range(2):
        for block, value in (
            (far[r], far_sum[r]), (missing[r], jnp.transpose(got_far[missing_slot[r]]))
        ):
            lanes_at = pl.ds(pl.multiple_of(BLOCK * (block - far_block), BLOCK), BLOCK)
            hi, lo = split(value)
            rows_hi[r * BLOCK : (r + 1) * BLOCK, lanes_at] = hi
            rows_lo[r * BLOCK : (r + 1) * BLOCK, lanes_at] = lo
    rows = (rows_hi[...], rows_lo[...])
    far_edges[...] = dot3(rows, (edge_hi[far_half, :], edge_lo[far_half, :]))
    far_gram = dot3((decay_t_hi[:, near_half], decay_t_lo[:, near_half]), rows)
    gram_hi, gram_lo = split(far_gram)
    stack = tuple(jnp.concatenate(pair, axis=0) for pair in ((rows[0], gram_hi), (rows[1], gram_lo)))
    for l in range(CLASSES):
        far_out[:, l * TILE : (l + 1) * TILE] = filtered(stack, l)

    in_low = core == 0
    tile_lane = iota((1, TILE), 1).astype(F32)
    rises = []
    for l in range(CLASSES):
        to_low = jnp.exp((tile_lane - TILE) * (1.0 / (1 + l)))
        to_high = jnp.exp((tile_lane + 1.0) * (-1.0 / (1 + l)))
        rises.append((jnp.where(in_low, to_low, to_high), jnp.where(in_low, to_high, to_low)))
    for k in range(2):
        y0 = k * BLOCK
        for d in range(REACH):
            copies[d, k + 1].wait_recv()
        if k == 0:
            corner = summed(3)
            blocks = (summed(2), corner)
            turned_corner[...] = jnp.transpose(corner)
        else:
            blocks = (turned_corner[...], summed(4))
        rows = split(jnp.concatenate(blocks, axis=1))
        here = pl.ds(pl.multiple_of(first + y0, BLOCK), BLOCK)
        decay_t = (decay_t_hi[:, here], decay_t_lo[:, here])
        edges = far_edges[y0 : y0 + BLOCK, :] + dot3(rows, (edge_hi[near_half, :], edge_lo[near_half, :]))
        mirror[...] += dot3(decay_t, split(edges))
        gram[...] += dot3(decay_t, rows)
        stack = rows
        if k == 1:
            near_gram = split(gram[...])
            stack = tuple(jnp.concatenate((a, b), axis=0) for a, b in zip(rows, near_gram))
        rims = []
        for lb in range(CLASSES):
            rim = edges[:, : 2 * BANDS] * filt_edge[lb, y0 : y0 + BLOCK, :]
            rims.append(rim[:, :BANDS] + rim[:, BANDS:])
        inside = jnp.concatenate([win_t[lb, :, here] for lb in range(CLASSES)], axis=1)
        hi, lo = split(jnp.concatenate(rims, axis=0))
        total[...] -= mm(inside, hi) + mm(inside, lo)
        for la in range(CLASSES):
            near_out = filtered(stack, la)
            above = inside[:, la * BLOCK :]
            tile = slice(la * TILE, (la + 1) * TILE)
            for j, half_cols in enumerate((near_half, far_half)):
                lane_col = 2 * BANDS + 2 * la + j

                def square(own, far_rows, source):
                    plain = near_out[own : own + BLOCK] if j == 0 else far_out[far_rows, tile]
                    return plain + source[:, lane_col : lane_col + 1] * rises[la][j]

                out = square(0, slice(y0, y0 + BLOCK), edges)
                hi, lo = split(
                    jnp.concatenate(
                        [out * filt[lb, y0 : y0 + BLOCK, half_cols] for lb in range(la, CLASSES)],
                        axis=0,
                    )
                )
                box = mm(above, hi) + mm(above, lo)
                if k == 1:
                    rim = square(BLOCK, slice(2 * BLOCK, 3 * BLOCK), mirror[...]) * outer[:, half_cols]
                    box = box - (rim[:BANDS] + rim[BANDS:])
                span = slice(la * PANEL + j * TILE, la * PANEL + (j + 1) * TILE)
                boxes[:, span] += box
    fisher = total[...]
    for la in range(CLASSES):
        for j, half_first in enumerate((first, TILE - first)):
            hi, lo = split(boxes[:, la * PANEL + j * TILE : la * PANEL + (j + 1) * TILE])
            channels = win[pl.ds(pl.multiple_of(la * PANEL + half_first, TILE), TILE), :]
            fisher = fisher + (mm(hi, channels) + mm(lo, channels))
    four = mirror[:, : 2 * BANDS] * outer_decay[...]
    fisher = fisher + (four[:BANDS, :BANDS] + four[:BANDS, BANDS:])
    fisher = fisher + (four[BANDS:, :BANDS] + four[BANDS:, BANDS:])
    row_class = iota((BANDS, BANDS), 0) % CLASSES
    col_class = iota((BANDS, BANDS), 1) % CLASSES
    kept = jnp.where(col_class <= row_class, fisher * SCALE, 0.0)
    wide = jnp.concatenate([kept, jnp.zeros_like(kept)], axis=1)
    turned_over = jnp.transpose(jnp.concatenate([wide, jnp.zeros_like(wide)], axis=0))
    fisher = kept + jnp.where(col_class > row_class, turned_over[:BANDS, :BANDS], 0.0)

    row = iota((BANDS // 2, BANDS), 0)
    owner = (row % 2) * 16 + row // 2
    col = iota((BANDS // 2, BANDS), 1)
    parts3 = []
    rest = fisher
    for _ in range(3):
        piece = rest.astype(BF16)
        parts3.append(piece)
        rest = rest - piece.astype(F32)
    turned = []
    for side in range(2):
        pick = jnp.where(col == 2 * owner + side, 1.0, 0.0).astype(BF16)
        turned.append(mm(pick, parts3[0]) + mm(pick, parts3[1]) + mm(pick, parts3[2]))
    placed = jnp.concatenate(turned, axis=1)
    for j in range(16):
        sum_xy[j] = placed[2 * j : 2 * j + 2]

    xy_copies = []
    for e in range(1, 16):
        copy = pltpu.make_async_remote_copy(
            src_ref=sum_xy.at[(plane + e) % 16], dst_ref=got_xy.at[e - 1],
            send_sem=xy_sem.at[0, e - 1], recv_sem=xy_sem.at[1, e - 1],
            device_id=plane_peer(e), device_id_type=MESH,
        )
        copy.start()
        xy_copies.append(copy)
    tile = sum_xy[plane]
    for e in range(15):
        xy_copies[e].wait_recv()
        tile = tile + got_xy[e]
    sum_z[0] = tile[0:1]
    sum_z[1] = tile[1:2]
    z_copies = []
    for e in range(1, 8):
        copy = pltpu.make_async_remote_copy(
            src_ref=sum_z.at[(spot + e) % 8 // 4], dst_ref=got_z.at[e - 1],
            send_sem=z_sem.at[0, e - 1], recv_sem=z_sem.at[1, e - 1],
            device_id=z_peer(e), device_id_type=MESH,
        )
        copy.start()
        z_copies.append(copy)
    mine = jnp.where(pos_z == 0, tile[0:1], tile[1:2])
    halves = [jnp.where(half == h, mine, 0.0) for h in range(2)]
    for e in range(7):
        z_copies[e].wait_recv()
        from_half = ((spot + 7 - e) % 8 % 4) // 2
        for h in range(2):
            halves[h] = halves[h] + jnp.where(from_half == h, got_z[e], 0.0)
    lanes = iota((16, 128), 1)
    band = 16 * part + iota((16, 128), 0)
    for h in range(2):
        line = jnp.broadcast_to(halves[h], (16, 128))
        for side in range(2):
            one = jnp.where(lanes == band + side * BANDS, line, 0.0)
            out_ref[h, :, side : side + 1] = jnp.sum(one, axis=1, keepdims=True)

    for copy in list(copies.values()) + [far_copy] + xy_copies + z_copies:
        copy.wait_send()


def body(*args):
    vmem = pltpu.VMEM
    dma = pltpu.SemaphoreType.DMA
    return pl.pallas_call(
        body_kernel,
        out_shape=jax.ShapeDtypeStruct((2, 16, 2), F32),
        in_specs=[
            pl.BlockSpec(memory_space=pltpu.HBM),
            pl.BlockSpec(memory_space=pltpu.HBM),
            pl.BlockSpec(memory_space=pltpu.HBM),
            pl.BlockSpec(memory_space=pltpu.HBM),
        ],
        out_specs=pl.BlockSpec(memory_space=pltpu.VMEM),
        scratch_shapes=[
            vmem((1, 2 * PANEL), jnp.int32),
            vmem((1, 2), jnp.int32),
            vmem((2, BANDS), jnp.int32),
            vmem((PANEL, PANEL), F32),
            vmem((5, BLOCK, BLOCK), F32),
            vmem((REACH, 5, BLOCK, BLOCK), F32),
            vmem((REACH, 1, 2 * PANEL), jnp.int32),
            vmem((REACH, 1, 2), jnp.int32),
            vmem((REACH, 2, BLOCK, BLOCK), F32),
            vmem((2, BLOCK, BLOCK), F32),
            vmem((2, BLOCK, BLOCK), F32),
            vmem((ROWS, 4 * BANDS), F32),
            vmem((ROWS + 2 * BANDS, CLASSES * TILE), F32),
            vmem((BLOCK, BLOCK), F32),
            vmem((ROWS, TILE), BF16),
            vmem((ROWS, TILE), BF16),
            vmem((PANEL, CLASSES * PANEL), BF16),
            vmem((PANEL, CLASSES * PANEL), BF16),
            vmem((PANEL, 4 * BANDS), BF16),
            vmem((PANEL, 4 * BANDS), BF16),
            vmem((CLASSES * PANEL, BANDS), BF16),
            vmem((PANEL, 2 * BANDS), BF16),
            vmem((PANEL, 2 * BANDS), BF16),
            vmem((2 * BANDS, PANEL), BF16),
            vmem((2 * BANDS, PANEL), BF16),
            vmem((2 * BANDS, PANEL), BF16),
            vmem((2 * BANDS, PANEL), BF16),
            vmem((CLASSES, BANDS, PANEL), BF16),
            vmem((PANEL, PANEL), BF16),
            vmem((PANEL, PANEL), BF16),
            vmem((CLASSES, ROWS, PANEL), F32),
            vmem((CLASSES, ROWS, 2 * BANDS), F32),
            vmem((2 * BANDS, PANEL), F32),
            vmem((2 * BANDS, 2 * BANDS), F32),
            vmem((BANDS, CLASSES * PANEL), F32),
            vmem((2 * BANDS, TILE), F32),
            vmem((BANDS, BANDS), F32),
            vmem((2 * BANDS, 4 * BANDS), F32),
            vmem((16, 2, 128), F32),
            vmem((15, 2, 128), F32),
            vmem((2, 1, 128), F32),
            vmem((7, 1, 128), F32),
            dma((REACH, len(MESSAGES))),
            dma((REACH, len(MESSAGES))),
            dma((2, REACH)),
            dma((2, REACH)),
            dma((2,)),
            dma((2,)),
            dma((9,)),
            dma((2, 15)),
            dma((2, 7)),
        ],
        compiler_params=pltpu.CompilerParams(
            collective_id=0, has_side_effects=True, vmem_limit_bytes=48 * 1024 * 1024
        ),
    )(*(pltpu.with_memory_space_constraint(x, pltpu.HBM) for x in args))


def solution(mesh):
    placed = (P("bl", "bp", None), P("bl", None), P("bl", None), P())
    return jax.shard_map(
        body, mesh=mesh, in_specs=placed, out_specs=P(None, "bp", "bl"), check_vma=False
    )
```

```python
import functools

import jax
import jax.numpy as jnp
from jax import lax
from jax.experimental import pallas as pl
from jax.experimental.pallas import tpu as pltpu
from jax.sharding import PartitionSpec as P

MESH = pl.DeviceIdType.MESH
F32 = jnp.float32
BF16 = jnp.bfloat16

GROUPS = 32
REACH = 4
SENDS = (-1, 2, -3, 4)
BLOCK = 128
TILE = 256
HALF = BLOCK // 2
PANEL = 512
ROWS = 256
BANDS = 64
WINDOW = 128
CLASSES = 4
SCALE = 1.0 / (4 * GROUPS * WINDOW)


def split(x):
    hi = x.astype(BF16)
    return hi, (x - hi.astype(F32)).astype(BF16)


def mm(a, b):
    return jnp.dot(a, b, preferred_element_type=F32)


def dot3(a, b):
    rows = a[0].shape[0]
    both = mm(jnp.concatenate(a, axis=0), b[0])
    return both[:rows] + (mm(a[0], b[1]) + both[rows:])


def iota(shape, dim):
    return lax.broadcasted_iota(jnp.int32, shape, dim)


def down(row, count):
    return jnp.transpose(jnp.broadcast_to(row, (128, count)))


def body_kernel(
    inv_ref, mask_hbm, partner_hbm, start_hbm, out_ref,
    mask_ref, partner_ref, start_ref, own_raw, own_pack, own_low, got, got_low, got_mask, got_partner, row_marks,
    far_sum, got_far, far_edges, far_out, filt_rise, outer_rise, turned_corner, rows_hi, rows_lo,
    toep_hi, toep_lo, edge_hi, edge_lo, win, decay_hi, decay_lo,
    decay_t_hi, decay_t_lo, edge_t_hi, edge_t_lo, win_t, panel_hi, panel_lo, filt, filt_edge,
    outer, outer_decay, boxes, gram, total, mirror,
    sum_xy, got_xy, sum_z, got_z,
    send_sem, recv_sem, mask_sem, partner_sem, sib_sem, far_sem, own_sem, xy_sem, z_sem,
):
    me = lax.axis_index("bl")
    part = lax.axis_index("bp")
    half = part // 2
    core = part % 2
    pos_z = me // 16
    first = pl.multiple_of(core * ROWS, ROWS)
    col0 = pl.multiple_of(half * PANEL, PANEL)
    sibling = (me, part + 1 - 2 * core)

    def by_core(zero, one):
        return core * (one - zero) + zero

    def target(d):
        return ((me + GROUPS + SENDS[d]) % GROUPS, part)

    def source(d):
        return ((me + GROUPS - SENDS[d]) % GROUPS, part)

    near = [2 * core, 2 * core + 1]
    far = [by_core(2 + r, 1 - r) for r in range(2)]
    missing = [by_core(3 - r, r) for r in range(2)]
    missing_slot = [by_core(1 - r, r) for r in range(2)]
    pack = [(0, far[0]), (1, far[1]), (0, near[0]), (0, near[1]), (1, near[1])]

    def lanes_of(block):
        return pl.ds(pl.multiple_of(col0 + BLOCK * block, BLOCK), BLOCK)

    plane = me % 16

    def plane_peer(e):
        return (me - plane + (plane + e) % 16, part)

    spot = pos_z * 4 + part

    def z_peer(e):
        g = (spot + e) % 8
        return (me % 16 + 16 * (g // 4), g % 4)

    peers = (
        [target(d) for d in range(REACH)]
        + [source(d) for d in range(REACH)]
        + [plane_peer(e) for e in range(1, 16)]
        + [z_peer(e) for e in range(1, 8)]
    )
    barrier = pltpu.get_barrier_semaphore()
    for peer in peers[: 2 * REACH]:
        pl.semaphore_signal(barrier, inc=1, device_id=peer, device_id_type=MESH)
    locals_ = [
        pltpu.make_async_copy(
            inv_ref.at[0, BLOCK * r : BLOCK * (r + 1), lanes_of(c)], own_pack.at[p], own_sem.at[p]
        )
        for p, (r, c) in enumerate(pack)
    ]
    own_rows = own_raw.at[pl.ds(first, ROWS)]
    locals_.append(
        pltpu.make_async_copy(inv_ref.at[0, :, pl.ds(col0, PANEL)], own_rows, own_sem.at[5])
    )
    locals_.append(pltpu.make_async_copy(mask_hbm, mask_ref, own_sem.at[6]))
    locals_.append(pltpu.make_async_copy(partner_hbm, partner_ref, own_sem.at[7]))
    locals_.append(pltpu.make_async_copy(start_hbm, start_ref, own_sem.at[8]))
    for copy in locals_:
        copy.start()
    for peer in peers[2 * REACH :]:
        pl.semaphore_signal(barrier, inc=1, device_id=peer, device_id_type=MESH)
    for n in (0, 1, 2, 4, 6, 7):
        locals_[n].wait()
    lower = iota((HALF // 2, BLOCK), 1) < HALF
    for n, p in enumerate((2, 4)):
        upper_rows = own_pack[p, HALF : HALF + HALF // 2, :]
        lower_rows = own_pack[p, HALF + HALF // 2 :, :]
        own_low[n] = jnp.where(lower, pltpu.roll(upper_rows, HALF, 1), lower_rows)
    pl.semaphore_wait(barrier, len(peers))

    mask_copies = []
    for d in range(REACH):
        pairs = [(mask_ref, got_mask, mask_sem)]
        if SENDS[d] > 0:
            pairs.append((partner_ref, got_partner, partner_sem))
        for src, dst, sem in pairs:
            copy = pltpu.make_async_remote_copy(
                src_ref=src, dst_ref=dst.at[d], send_sem=sem.at[0, d], recv_sem=sem.at[1, d],
                device_id=target(d), device_id_type=MESH,
            )
            copy.start()
            mask_copies.append(copy)
    copies = {}
    pieces = (
        ((own_pack.at[pl.ds(0, 2)], lambda d: got.at[d, pl.ds(0, 2)]),),
        (
            (own_pack.at[3], lambda d: got.at[d, 3]),
            (own_pack.at[2, pl.ds(0, HALF)], lambda d: got.at[d, 2, pl.ds(0, HALF)]),
            (own_low.at[0], lambda d: got_low.at[d, 0]),
        ),
        (
            (own_pack.at[4, pl.ds(0, HALF)], lambda d: got.at[d, 4, pl.ds(0, HALF)]),
            (own_low.at[1], lambda d: got_low.at[d, 1]),
        ),
    )
    sem_id = 0
    for g, group in enumerate(pieces):
        if g == 1:
            locals_[3].wait()
        for src, dst in group:
            for d in range(REACH):
                copy = pltpu.make_async_remote_copy(
                    src_ref=src, dst_ref=dst(d),
                    send_sem=send_sem.at[d, sem_id], recv_sem=recv_sem.at[d, sem_id],
                    device_id=target(d), device_id_type=MESH,
                )
                copy.start()
                copies.setdefault(g, []).append(copy)
            sem_id += 1
    locals_[5].wait()
    sib_copy = pltpu.make_async_remote_copy(
        src_ref=own_rows, dst_ref=own_rows,
        send_sem=sib_sem.at[0], recv_sem=sib_sem.at[1], device_id=sibling, device_id_type=MESH,
    )
    sib_copy.start()

    locals_[8].wait()
    starts = start_ref[pl.ds(half, 1), :]
    starts2 = jnp.concatenate([starts, starts], axis=1)
    lane = iota((1, 2 * BANDS), 1)
    lane_class = lane % CLASSES
    rate = 1.0 / (1 + lane_class).astype(F32)
    is_left = lane < BANDS
    for r0 in range(0, PANEL, 128):
        pos = iota((128, 2 * BANDS), 0) + r0
        from_start = pos - starts2
        to_end = starts2 + (WINDOW - 1) - pos
        inside = (from_start >= 0) & (to_end >= 0)
        gap = jnp.where(is_left, -from_start, -to_end)
        edge = jnp.where(gap > 0, jnp.exp(-jnp.abs(gap).astype(F32) * rate), 0.0)
        edge_hi[r0 : r0 + 128, : 2 * BANDS], edge_lo[r0 : r0 + 128, : 2 * BANDS] = split(edge)
        side_lane = iota((128, 2 * BANDS), 1)
        per_band = side_lane >= BANDS
        odd = jnp.where(per_band, 1, side_lane % 2)
        side_class = jnp.where(per_band, side_lane, side_lane // 2) % CLASSES
        reach = jnp.where((odd + core) % 2 == 1, TILE - 1 - pos, pos - TILE)
        side_rate = 1.0 / (1 + side_class).astype(F32)
        used = per_band | (side_lane < 2 * CLASSES)
        spill = jnp.where(
            (reach >= 0) & used, jnp.exp(-jnp.abs(reach).astype(F32) * side_rate), 0.0
        )
        edge_hi[r0 : r0 + 128, 2 * BANDS :], edge_lo[r0 : r0 + 128, 2 * BANDS :] = split(spill)
        decay = jnp.where(inside, jnp.exp(-jnp.abs(gap).astype(F32) * rate), 0.0)
        decay_hi[r0 : r0 + 128, :], decay_lo[r0 : r0 + 128, :] = split(decay)
        for l in range(CLASSES):
            one = jnp.where(inside & (lane_class == l), 1.0, 0.0)[:, :BANDS]
            win[l * PANEL + r0 : l * PANEL + r0 + 128, :] = one.astype(BF16)
    starts_t = down(starts2.astype(F32), 2 * BANDS).astype(jnp.int32)
    sub = iota((2 * BANDS, 128), 0)
    sub_class = sub % CLASSES
    rate_t = 1.0 / (1 + sub_class).astype(F32)
    is_left_t = sub < BANDS
    for r0 in range(0, PANEL, 128):
        pos = iota((2 * BANDS, 128), 1) + r0
        from_start = pos - starts_t
        to_end = starts_t + (WINDOW - 1) - pos
        inside = (from_start >= 0) & (to_end >= 0)
        gap = jnp.where(is_left_t, -from_start, -to_end)
        weight = jnp.exp(-jnp.abs(gap).astype(F32) * rate_t)
        edge_t_hi[:, r0 : r0 + 128], edge_t_lo[:, r0 : r0 + 128] = split(
            jnp.where(gap > 0, weight, 0.0)
        )
        decay_t_hi[:, r0 : r0 + 128], decay_t_lo[:, r0 : r0 + 128] = split(
            jnp.where(inside, weight, 0.0)
        )
        for l in range(CLASSES):
            one = jnp.where(inside & (sub_class == l), 1.0, 0.0)[:BANDS, :]
            win_t[l, :, r0 : r0 + 128] = one.astype(BF16)

    def fill(block, carry):
        r0 = pl.multiple_of(block * 128, 128)
        dist = jnp.abs(iota((128, PANEL), 0) + r0 - iota((128, PANEL), 1)).astype(F32)
        for l in range(CLASSES):
            hi, lo = split(jnp.exp(dist * (-1.0 / (1 + l))))
            toep_hi[pl.ds(r0, 128), l * PANEL : (l + 1) * PANEL] = hi
            toep_lo[pl.ds(r0, 128), l * PANEL : (l + 1) * PANEL] = lo
        return carry

    lax.fori_loop(0, PANEL // 128, fill, 0)

    sib_copy.wait()
    cols = mask_ref[:, pl.ds(col0, PANEL)].astype(F32)
    for r0 in range(0, PANEL, 128):
        marks = down(cols[:, r0 : r0 + 128], 128)
        for c0 in range(0, PANEL, 128):
            block = own_raw[r0 : r0 + 128, c0 : c0 + 128] * marks * cols[:, c0 : c0 + 128]
            panel_hi[r0 : r0 + 128, c0 : c0 + 128], panel_lo[r0 : r0 + 128, c0 : c0 + 128] = split(
                block
            )
    panel = (panel_hi[...], panel_lo[...])
    decays = (decay_hi[...], decay_lo[...])
    for l in range(CLASSES):
        rows = (
            toep_hi[pl.ds(first, ROWS), l * PANEL : (l + 1) * PANEL],
            toep_lo[pl.ds(first, ROWS), l * PANEL : (l + 1) * PANEL],
        )
        out = dot3(rows, panel)
        filt[l] = out
        filt_edge[l] = dot3(split(out), decays)
    outer[...] = dot3((edge_t_hi[...], edge_t_lo[...]), panel)
    outer_decay[...] = dot3(split(outer[...]), decays)

    near_half = pl.ds(first, TILE)
    far_half = pl.ds(pl.multiple_of(TILE - first, TILE), TILE)
    far_pos = iota((TILE, BANDS), 0)
    far_dist = jnp.where(core == 0, far_pos + 1, TILE - far_pos).astype(F32)
    far_rise = jnp.exp(-far_dist / (1 + iota((TILE, BANDS), 1) % CLASSES).astype(F32))
    any_win = 0.0
    for l in range(CLASSES):
        start = pl.multiple_of(l * PANEL + TILE - first, TILE)
        any_win = any_win + win[pl.ds(start, TILE), :].astype(F32)
    far_rise = split(far_rise * any_win)
    for lb in range(CLASSES):
        filt_rise[lb] = dot3(split(filt[lb, :, far_half]), far_rise)
    outer_rise[...] = dot3(split(outer[:, far_half]), far_rise)
    for copy in mask_copies:
        copy.wait()
    gram[...] = jnp.zeros_like(gram)
    mirror[...] = jnp.zeros_like(mirror)
    for d in range(REACH):
        if SENDS[d] < 0:
            hits = jnp.where(partner_ref[...] == source(d)[0], 1.0, 0.0)
        else:
            hits = jnp.where(got_partner[d] == me, 1.0, 0.0)
        weight = hits[:, 0:1] + hits[:, 1:2]
        for r in range(2):
            marks = got_mask[d, :, lanes_of(near[r])].astype(F32) * weight
            row_marks[d, r] = down(marks, BLOCK)

    def summed(p):
        r, c = pack[p]
        out = 0.0
        for d in range(REACH):
            cols = got_mask[d, :, lanes_of(c)].astype(F32)
            out = out + got[d, p] * row_marks[d, r] * cols
        return out

    def summed_square(p, n):
        r, c = pack[p]
        top = low = 0.0
        for d in range(REACH):
            cols = got_mask[d, :, lanes_of(c)].astype(F32)
            low_cols = jnp.where(lower[:1], pltpu.roll(cols, HALF, 1), cols)
            marks = row_marks[d, r]
            low_marks = jnp.where(lower, marks[HALF : HALF + HALF // 2], marks[HALF + HALF // 2 :])
            top = top + got[d, p, :HALF] * marks[:HALF] * cols
            low = low + got_low[d, n] * low_marks * low_cols
        square = jnp.concatenate((top, pltpu.roll(low, HALF, 1), low), axis=0)
        row, lane_at = iota((BLOCK, BLOCK), 0), iota((BLOCK, BLOCK), 1)
        return jnp.where((row >= HALF) & (lane_at < HALF), jnp.transpose(square), square)

    def filtered(rows, l):
        square = slice(l * PANEL, l * PANEL + TILE)
        return dot3(rows, (toep_hi[:TILE, square], toep_lo[:TILE, square]))

    far_copy = pltpu.make_async_remote_copy(
        src_ref=far_sum, dst_ref=got_far,
        send_sem=far_sem.at[0], recv_sem=far_sem.at[1], device_id=sibling, device_id_type=MESH,
    )
    for copy in copies[0]:
        copy.wait_recv()
    for r in range(2):
        far_sum[r] = summed(r)
    far_copy.start()
    far_copy.wait_recv()
    far_block = 2 - 2 * core
    for r in range(2):
        for block, value in (
            (far[r], far_sum[r]), (missing[r], jnp.transpose(got_far[missing_slot[r]]))
        ):
            lanes_at = pl.ds(pl.multiple_of(BLOCK * (block - far_block), BLOCK), BLOCK)
            hi, lo = split(value)
            rows_hi[r * BLOCK : (r + 1) * BLOCK, lanes_at] = hi
            rows_lo[r * BLOCK : (r + 1) * BLOCK, lanes_at] = lo
    rows = (rows_hi[...], rows_lo[...])
    far_edges[...] = dot3(rows, (edge_hi[far_half, :], edge_lo[far_half, :]))
    far_gram = dot3((decay_t_hi[:, near_half], decay_t_lo[:, near_half]), rows)
    gram_hi, gram_lo = split(far_gram)
    stack = tuple(jnp.concatenate(pair, axis=0) for pair in ((rows[0], gram_hi), (rows[1], gram_lo)))
    for l in range(CLASSES):
        far_out[:, l * TILE : (l + 1) * TILE] = filtered(stack, l)
    inside_all = jnp.concatenate([win_t[lb, :, near_half] for lb in range(CLASSES)], axis=1)
    for la in range(CLASSES):
        out = far_out[:ROWS, la * TILE : (la + 1) * TILE]
        hi, lo = split(
            jnp.concatenate([out * filt[lb, :, far_half] for lb in range(la, CLASSES)], axis=0)
        )
        above = inside_all[:, la * ROWS :]
        rim = far_out[ROWS:, la * TILE : (la + 1) * TILE] * outer[:, far_half]
        box = mm(above, hi) + mm(above, lo) - (rim[:BANDS] + rim[BANDS:])
        boxes[:, la * TILE : (la + 1) * TILE] = box
    far_fisher = jnp.zeros((BANDS, BANDS), F32)
    for la in range(CLASSES):
        hi, lo = split(boxes[:, la * TILE : (la + 1) * TILE])
        channels = win[pl.ds(pl.multiple_of(la * PANEL + TILE - first, TILE), TILE), :]
        far_fisher = far_fisher + (mm(hi, channels) + mm(lo, channels))
    total[...] = far_fisher

    in_low = core == 0
    tile_lane = iota((1, TILE), 1).astype(F32)
    rises = []
    for l in range(CLASSES):
        to_low = jnp.exp((tile_lane - TILE) * (1.0 / (1 + l)))
        to_high = jnp.exp((tile_lane + 1.0) * (-1.0 / (1 + l)))
        rises.append(jnp.where(in_low, to_low, to_high))
    for k in range(2):
        y0 = k * BLOCK
        for copy in copies[k + 1]:
            copy.wait_recv()
        if k == 0:
            corner = summed(3)
            blocks = (summed_square(2, 0), corner)
            turned_corner[...] = jnp.transpose(corner)
        else:
            blocks = (turned_corner[...], summed_square(4, 1))
        rows = split(jnp.concatenate(blocks, axis=1))
        here = pl.ds(pl.multiple_of(first + y0, BLOCK), BLOCK)
        decay_t = (decay_t_hi[:, here], decay_t_lo[:, here])
        edges = far_edges[y0 : y0 + BLOCK, :] + dot3(rows, (edge_hi[near_half, :], edge_lo[near_half, :]))
        mirror[...] += dot3(decay_t, split(edges))
        gram[...] += dot3(decay_t, rows)
        stack = rows
        if k == 1:
            near_gram = split(gram[...])
            stack = tuple(jnp.concatenate((a, b), axis=0) for a, b in zip(rows, near_gram))
        rims = []
        for lb in range(CLASSES):
            rim = edges[:, : 2 * BANDS] * filt_edge[lb, y0 : y0 + BLOCK, :]
            spilt = edges[:, 3 * BANDS :] * filt_rise[lb, y0 : y0 + BLOCK, :]
            rims.append(rim[:, :BANDS] + rim[:, BANDS:] - spilt)
        inside = jnp.concatenate([win_t[lb, :, here] for lb in range(CLASSES)], axis=1)
        hi, lo = split(jnp.concatenate(rims, axis=0))
        total[...] -= mm(inside, hi) + mm(inside, lo)
        for la in range(CLASSES):
            near_out = filtered(stack, la)
            above = inside[:, la * BLOCK :]
            step_up = rises[la]
            lane_col = 2 * BANDS + 2 * la
            out = near_out[:BLOCK] + edges[:, lane_col : lane_col + 1] * step_up
            hi, lo = split(
                jnp.concatenate(
                    [out * filt[lb, y0 : y0 + BLOCK, near_half] for lb in range(la, CLASSES)], axis=0
                )
            )
            box = mm(above, hi) + mm(above, lo)
            span = slice(la * TILE, (la + 1) * TILE)
            if k == 0:
                boxes[:, span] = box
            else:
                rim = near_out[BLOCK:] + mirror[:, lane_col : lane_col + 1] * step_up
                rim = rim * outer[:, near_half]
                boxes[:, span] += box - (rim[:BANDS] + rim[BANDS:])
    fisher = total[...]
    for la in range(CLASSES):
        hi, lo = split(boxes[:, la * TILE : (la + 1) * TILE])
        channels = win[pl.ds(pl.multiple_of(la * PANEL + first, TILE), TILE), :]
        fisher = fisher + (mm(hi, channels) + mm(lo, channels))
    over = mirror[:, 3 * BANDS :] * outer_rise[...]
    fisher = fisher - (over[:BANDS] + over[BANDS:])
    four = mirror[:, : 2 * BANDS] * outer_decay[...]
    fisher = fisher + (four[:BANDS, :BANDS] + four[:BANDS, BANDS:])
    fisher = fisher + (four[BANDS:, :BANDS] + four[BANDS:, BANDS:])
    row_class = iota((BANDS, BANDS), 0) % CLASSES
    col_class = iota((BANDS, BANDS), 1) % CLASSES
    kept = jnp.where(col_class <= row_class, fisher * SCALE, 0.0)
    wide = jnp.concatenate([kept, jnp.zeros_like(kept)], axis=1)
    turned_over = jnp.transpose(jnp.concatenate([wide, jnp.zeros_like(wide)], axis=0))
    fisher = kept + jnp.where(col_class > row_class, turned_over[:BANDS, :BANDS], 0.0)

    row = iota((BANDS // 2, BANDS), 0)
    owner = (row % 2) * 16 + row // 2
    col = iota((BANDS // 2, BANDS), 1)
    parts3 = []
    rest = fisher
    for _ in range(3):
        piece = rest.astype(BF16)
        parts3.append(piece)
        rest = rest - piece.astype(F32)
    turned = []
    for side in range(2):
        pick = jnp.where(col == 2 * owner + side, 1.0, 0.0).astype(BF16)
        turned.append(mm(pick, parts3[0]) + mm(pick, parts3[1]) + mm(pick, parts3[2]))
    placed = jnp.concatenate(turned, axis=1)
    for j in range(16):
        sum_xy[j] = placed[2 * j : 2 * j + 2]

    xy_copies = []
    for e in range(1, 16):
        copy = pltpu.make_async_remote_copy(
            src_ref=sum_xy.at[(plane + e) % 16], dst_ref=got_xy.at[e - 1],
            send_sem=xy_sem.at[0, e - 1], recv_sem=xy_sem.at[1, e - 1],
            device_id=plane_peer(e), device_id_type=MESH,
        )
        copy.start()
        xy_copies.append(copy)
    tile = sum_xy[plane]
    for e in range(15):
        xy_copies[e].wait_recv()
        tile = tile + got_xy[e]
    sum_z[0] = tile[0:1]
    sum_z[1] = tile[1:2]
    z_copies = []
    for e in range(1, 8):
        copy = pltpu.make_async_remote_copy(
            src_ref=sum_z.at[(spot + e) % 8 // 4], dst_ref=got_z.at[e - 1],
            send_sem=z_sem.at[0, e - 1], recv_sem=z_sem.at[1, e - 1],
            device_id=z_peer(e), device_id_type=MESH,
        )
        copy.start()
        z_copies.append(copy)
    mine = jnp.where(pos_z == 0, tile[0:1], tile[1:2])
    halves = [jnp.where(half == h, mine, 0.0) for h in range(2)]
    for e in range(7):
        z_copies[e].wait_recv()
        from_half = ((spot + 7 - e) % 8 % 4) // 2
        for h in range(2):
            halves[h] = halves[h] + jnp.where(from_half == h, got_z[e], 0.0)
    lanes = iota((16, 128), 1)
    band = 16 * part + iota((16, 128), 0)
    for h in range(2):
        line = jnp.broadcast_to(halves[h], (16, 128))
        for side in range(2):
            one = jnp.where(lanes == band + side * BANDS, line, 0.0)
            out_ref[h, :, side : side + 1] = jnp.sum(one, axis=1, keepdims=True)

    for copy in copies[0] + copies[1] + copies[2] + [far_copy] + xy_copies + z_copies:
        copy.wait_send()


def body(*args):
    vmem = pltpu.VMEM
    dma = pltpu.SemaphoreType.DMA
    return pl.pallas_call(
        body_kernel,
        out_shape=jax.ShapeDtypeStruct((2, 16, 2), F32),
        in_specs=[
            pl.BlockSpec(memory_space=pltpu.HBM),
            pl.BlockSpec(memory_space=pltpu.HBM),
            pl.BlockSpec(memory_space=pltpu.HBM),
            pl.BlockSpec(memory_space=pltpu.HBM),
        ],
        out_specs=pl.BlockSpec(memory_space=pltpu.VMEM),
        scratch_shapes=[
            vmem((1, 2 * PANEL), jnp.int32),
            vmem((1, 2), jnp.int32),
            vmem((2, BANDS), jnp.int32),
            vmem((PANEL, PANEL), F32),
            vmem((5, BLOCK, BLOCK), F32),
            vmem((2, HALF // 2, BLOCK), F32),
            vmem((REACH, 5, BLOCK, BLOCK), F32),
            vmem((REACH, 2, HALF // 2, BLOCK), F32),
            vmem((REACH, 1, 2 * PANEL), jnp.int32),
            vmem((REACH, 1, 2), jnp.int32),
            vmem((REACH, 2, BLOCK, BLOCK), F32),
            vmem((2, BLOCK, BLOCK), F32),
            vmem((2, BLOCK, BLOCK), F32),
            vmem((ROWS, 4 * BANDS), F32),
            vmem((ROWS + 2 * BANDS, CLASSES * TILE), F32),
            vmem((CLASSES, ROWS, BANDS), F32),
            vmem((2 * BANDS, BANDS), F32),
            vmem((BLOCK, BLOCK), F32),
            vmem((ROWS, TILE), BF16),
            vmem((ROWS, TILE), BF16),
            vmem((PANEL, CLASSES * PANEL), BF16),
            vmem((PANEL, CLASSES * PANEL), BF16),
            vmem((PANEL, 4 * BANDS), BF16),
            vmem((PANEL, 4 * BANDS), BF16),
            vmem((CLASSES * PANEL, BANDS), BF16),
            vmem((PANEL, 2 * BANDS), BF16),
            vmem((PANEL, 2 * BANDS), BF16),
            vmem((2 * BANDS, PANEL), BF16),
            vmem((2 * BANDS, PANEL), BF16),
            vmem((2 * BANDS, PANEL), BF16),
            vmem((2 * BANDS, PANEL), BF16),
            vmem((CLASSES, BANDS, PANEL), BF16),
            vmem((PANEL, PANEL), BF16),
            vmem((PANEL, PANEL), BF16),
            vmem((CLASSES, ROWS, PANEL), F32),
            vmem((CLASSES, ROWS, 2 * BANDS), F32),
            vmem((2 * BANDS, PANEL), F32),
            vmem((2 * BANDS, 2 * BANDS), F32),
            vmem((BANDS, CLASSES * TILE), F32),
            vmem((2 * BANDS, TILE), F32),
            vmem((BANDS, BANDS), F32),
            vmem((2 * BANDS, 4 * BANDS), F32),
            vmem((16, 2, 128), F32),
            vmem((15, 2, 128), F32),
            vmem((2, 1, 128), F32),
            vmem((7, 1, 128), F32),
            dma((REACH, 6)),
            dma((REACH, 6)),
            dma((2, REACH)),
            dma((2, REACH)),
            dma((2,)),
            dma((2,)),
            dma((9,)),
            dma((2, 15)),
            dma((2, 7)),
        ],
        compiler_params=pltpu.CompilerParams(
            collective_id=0, has_side_effects=True, vmem_limit_bytes=48 * 1024 * 1024
        ),
    )(*(pltpu.with_memory_space_constraint(x, pltpu.HBM) for x in args))


def solution(mesh):
    placed = (P("bl", "bp", None), P("bl", None), P("bl", None), P())
    return jax.shard_map(
        body, mesh=mesh, in_specs=placed, out_specs=P(None, "bp", "bl"), check_vma=False
    )
```

```python
import functools

import jax
import jax.numpy as jnp
from jax import lax
from jax.experimental import pallas as pl
from jax.experimental.pallas import tpu as pltpu
from jax.sharding import PartitionSpec as P

MESH = pl.DeviceIdType.MESH
F32 = jnp.float32
BF16 = jnp.bfloat16

GROUPS = 32
REACH = 4
SENDS = (-1, 2, -3, 4)
BLOCK = 128
TILE = 256
HALF = BLOCK // 2
PANEL = 512
ROWS = 256
BANDS = 64
WINDOW = 128
CLASSES = 4
SCALE = 1.0 / (4 * GROUPS * WINDOW)


def split(x):
    hi = x.astype(BF16)
    return hi, (x - hi.astype(F32)).astype(BF16)


def mm(a, b):
    return jnp.dot(a, b, preferred_element_type=F32)


def dot3(a, b):
    rows = a[0].shape[0]
    both = mm(jnp.concatenate(a, axis=0), b[0])
    return both[:rows] + (mm(a[0], b[1]) + both[rows:])


def iota(shape, dim):
    return lax.broadcasted_iota(jnp.int32, shape, dim)


def down(row, count):
    return jnp.transpose(jnp.broadcast_to(row, (128, count)))


def band_at(place):
    return 2 * ((place % 2) * 16 + (place % 32) // 2) + (place // 32) % 2


def class_at(place):
    return 2 * ((place // 2) % 2) + (place // 32) % 2


def body_kernel(
    inv_ref, mask_hbm, partner_hbm, start_hbm, out_ref,
    mask_ref, partner_ref, start_ref, own_raw, own_pack, own_low, got, got_low, got_mask, got_partner, row_marks,
    far_sum, got_far, far_edges, far_out, filt_rise, outer_rise, turned_corner, rows_hi, rows_lo,
    toep_hi, toep_lo, edge_hi, edge_lo, win, decay_hi, decay_lo,
    decay_t_hi, decay_t_lo, edge_t_hi, edge_t_lo, win_t, panel_hi, panel_lo, filt, filt_edge,
    outer, outer_decay, boxes, gram, total, mirror,
    sum_xy, got_xy, sum_z, got_z,
    send_sem, recv_sem, mask_sem, partner_sem, sib_sem, far_sem, own_sem, xy_sem, z_sem,
):
    me = lax.axis_index("bl")
    part = lax.axis_index("bp")
    half = part // 2
    core = part % 2
    pos_z = me // 16
    first = pl.multiple_of(core * ROWS, ROWS)
    col0 = pl.multiple_of(half * PANEL, PANEL)
    sibling = (me, part + 1 - 2 * core)

    def by_core(zero, one):
        return core * (one - zero) + zero

    def target(d):
        return ((me + GROUPS + SENDS[d]) % GROUPS, part)

    def source(d):
        return ((me + GROUPS - SENDS[d]) % GROUPS, part)

    near = [2 * core, 2 * core + 1]
    far = [by_core(2 + r, 1 - r) for r in range(2)]
    missing = [by_core(3 - r, r) for r in range(2)]
    missing_slot = [by_core(1 - r, r) for r in range(2)]
    pack = [(0, far[0]), (1, far[1]), (0, near[0]), (0, near[1]), (1, near[1])]

    def lanes_of(block):
        return pl.ds(pl.multiple_of(col0 + BLOCK * block, BLOCK), BLOCK)

    plane = me % 16

    def plane_peer(e):
        return (me - plane + (plane + e) % 16, part)

    spot = pos_z * 4 + part

    def z_peer(e):
        g = (spot + e) % 8
        return (me % 16 + 16 * (g // 4), g % 4)

    peers = (
        [target(d) for d in range(REACH)]
        + [source(d) for d in range(REACH)]
        + [plane_peer(e) for e in range(1, 16)]
        + [z_peer(e) for e in range(1, 8)]
    )
    barrier = pltpu.get_barrier_semaphore()
    for peer in peers[: 2 * REACH]:
        pl.semaphore_signal(barrier, inc=1, device_id=peer, device_id_type=MESH)
    locals_ = [
        pltpu.make_async_copy(
            inv_ref.at[0, BLOCK * r : BLOCK * (r + 1), lanes_of(c)], own_pack.at[p], own_sem.at[p]
        )
        for p, (r, c) in enumerate(pack)
    ]
    own_rows = own_raw.at[pl.ds(first, ROWS)]
    locals_.append(
        pltpu.make_async_copy(inv_ref.at[0, :, pl.ds(col0, PANEL)], own_rows, own_sem.at[5])
    )
    locals_.append(pltpu.make_async_copy(mask_hbm, mask_ref, own_sem.at[6]))
    locals_.append(pltpu.make_async_copy(partner_hbm, partner_ref, own_sem.at[7]))
    locals_.append(pltpu.make_async_copy(start_hbm, start_ref, own_sem.at[8]))
    for copy in locals_:
        copy.start()
    for peer in peers[2 * REACH :]:
        pl.semaphore_signal(barrier, inc=1, device_id=peer, device_id_type=MESH)
    for n in (0, 1, 2, 4, 6, 7):
        locals_[n].wait()
    lower = iota((HALF // 2, BLOCK), 1) < HALF
    for n, p in enumerate((2, 4)):
        upper_rows = own_pack[p, HALF : HALF + HALF // 2, :]
        lower_rows = own_pack[p, HALF + HALF // 2 :, :]
        own_low[n] = jnp.where(lower, pltpu.roll(upper_rows, HALF, 1), lower_rows)
    pl.semaphore_wait(barrier, len(peers))

    mask_copies = []
    for d in range(REACH):
        pairs = [(mask_ref, got_mask, mask_sem)]
        if SENDS[d] > 0:
            pairs.append((partner_ref, got_partner, partner_sem))
        for src, dst, sem in pairs:
            copy = pltpu.make_async_remote_copy(
                src_ref=src, dst_ref=dst.at[d], send_sem=sem.at[0, d], recv_sem=sem.at[1, d],
                device_id=target(d), device_id_type=MESH,
            )
            copy.start()
            mask_copies.append(copy)
    copies = {}
    pieces = (
        ((own_pack.at[pl.ds(0, 2)], lambda d: got.at[d, pl.ds(0, 2)]),),
        (
            (own_pack.at[3], lambda d: got.at[d, 3]),
            (own_pack.at[2, pl.ds(0, HALF)], lambda d: got.at[d, 2, pl.ds(0, HALF)]),
            (own_low.at[0], lambda d: got_low.at[d, 0]),
        ),
        (
            (own_pack.at[4, pl.ds(0, HALF)], lambda d: got.at[d, 4, pl.ds(0, HALF)]),
            (own_low.at[1], lambda d: got_low.at[d, 1]),
        ),
    )
    sem_id = 0
    for g, group in enumerate(pieces):
        if g == 1:
            locals_[3].wait()
        for src, dst in group:
            for d in range(REACH):
                copy = pltpu.make_async_remote_copy(
                    src_ref=src, dst_ref=dst(d),
                    send_sem=send_sem.at[d, sem_id], recv_sem=recv_sem.at[d, sem_id],
                    device_id=target(d), device_id_type=MESH,
                )
                copy.start()
                copies.setdefault(g, []).append(copy)
            sem_id += 1
    locals_[5].wait()
    sib_copy = pltpu.make_async_remote_copy(
        src_ref=own_rows, dst_ref=own_rows,
        send_sem=sib_sem.at[0], recv_sem=sib_sem.at[1], device_id=sibling, device_id_type=MESH,
    )
    sib_copy.start()

    locals_[8].wait()
    starts = start_ref[pl.ds(half, 1), :]
    starts2 = jnp.concatenate([starts, starts], axis=1)
    square = (2 * BANDS, 2 * BANDS)
    in_place = iota(square, 0) == band_at(iota(square, 1))
    by_band = down(starts2.astype(F32), 2 * BANDS)
    starts2 = jnp.sum(jnp.where(in_place, by_band, 0.0), axis=0, keepdims=True).astype(jnp.int32)
    lane = iota((1, 2 * BANDS), 1)
    lane_class = class_at(lane)
    rate = 1.0 / (1 + lane_class).astype(F32)
    is_left = lane < BANDS
    for r0 in range(0, PANEL, 128):
        pos = iota((128, 2 * BANDS), 0) + r0
        from_start = pos - starts2
        to_end = starts2 + (WINDOW - 1) - pos
        inside = (from_start >= 0) & (to_end >= 0)
        gap = jnp.where(is_left, -from_start, -to_end)
        edge = jnp.where(gap > 0, jnp.exp(-jnp.abs(gap).astype(F32) * rate), 0.0)
        edge_hi[r0 : r0 + 128, : 2 * BANDS], edge_lo[r0 : r0 + 128, : 2 * BANDS] = split(edge)
        side_lane = iota((128, 2 * BANDS), 1)
        per_band = side_lane >= BANDS
        odd = jnp.where(per_band, 1, side_lane % 2)
        side_class = jnp.where(per_band, class_at(side_lane), side_lane // 2 % CLASSES)
        reach = jnp.where((odd + core) % 2 == 1, TILE - 1 - pos, pos - TILE)
        side_rate = 1.0 / (1 + side_class).astype(F32)
        used = per_band | (side_lane < 2 * CLASSES)
        spill = jnp.where(
            (reach >= 0) & used, jnp.exp(-jnp.abs(reach).astype(F32) * side_rate), 0.0
        )
        edge_hi[r0 : r0 + 128, 2 * BANDS :], edge_lo[r0 : r0 + 128, 2 * BANDS :] = split(spill)
        decay = jnp.where(inside, jnp.exp(-jnp.abs(gap).astype(F32) * rate), 0.0)
        decay_hi[r0 : r0 + 128, :], decay_lo[r0 : r0 + 128, :] = split(decay)
        for l in range(CLASSES):
            one = jnp.where(inside & (lane_class == l), 1.0, 0.0)[:, :BANDS]
            win[l * PANEL + r0 : l * PANEL + r0 + 128, :] = one.astype(BF16)
    starts_t = down(starts2.astype(F32), 2 * BANDS).astype(jnp.int32)
    sub = iota((2 * BANDS, 128), 0)
    sub_class = class_at(sub)
    rate_t = 1.0 / (1 + sub_class).astype(F32)
    is_left_t = sub < BANDS
    for r0 in range(0, PANEL, 128):
        pos = iota((2 * BANDS, 128), 1) + r0
        from_start = pos - starts_t
        to_end = starts_t + (WINDOW - 1) - pos
        inside = (from_start >= 0) & (to_end >= 0)
        gap = jnp.where(is_left_t, -from_start, -to_end)
        weight = jnp.exp(-jnp.abs(gap).astype(F32) * rate_t)
        edge_t_hi[:, r0 : r0 + 128], edge_t_lo[:, r0 : r0 + 128] = split(
            jnp.where(gap > 0, weight, 0.0)
        )
        decay_t_hi[:, r0 : r0 + 128], decay_t_lo[:, r0 : r0 + 128] = split(
            jnp.where(inside, weight, 0.0)
        )
        for l in range(CLASSES):
            one = jnp.where(inside & (sub_class == l), 1.0, 0.0)[:BANDS, :]
            win_t[l, :, r0 : r0 + 128] = one.astype(BF16)

    def fill(block, carry):
        r0 = pl.multiple_of(block * 128, 128)
        dist = jnp.abs(iota((128, PANEL), 0) + r0 - iota((128, PANEL), 1)).astype(F32)
        for l in range(CLASSES):
            hi, lo = split(jnp.exp(dist * (-1.0 / (1 + l))))
            toep_hi[pl.ds(r0, 128), l * PANEL : (l + 1) * PANEL] = hi
            toep_lo[pl.ds(r0, 128), l * PANEL : (l + 1) * PANEL] = lo
        return carry

    lax.fori_loop(0, PANEL // 128, fill, 0)

    sib_copy.wait()
    cols = mask_ref[:, pl.ds(col0, PANEL)].astype(F32)
    for r0 in range(0, PANEL, 128):
        marks = down(cols[:, r0 : r0 + 128], 128)
        for c0 in range(0, PANEL, 128):
            block = own_raw[r0 : r0 + 128, c0 : c0 + 128] * marks * cols[:, c0 : c0 + 128]
            panel_hi[r0 : r0 + 128, c0 : c0 + 128], panel_lo[r0 : r0 + 128, c0 : c0 + 128] = split(
                block
            )
    panel = (panel_hi[...], panel_lo[...])
    decays = (decay_hi[...], decay_lo[...])
    for l in range(CLASSES):
        rows = (
            toep_hi[pl.ds(first, ROWS), l * PANEL : (l + 1) * PANEL],
            toep_lo[pl.ds(first, ROWS), l * PANEL : (l + 1) * PANEL],
        )
        out = dot3(rows, panel)
        filt[l] = out
        filt_edge[l] = dot3(split(out), decays)
    outer[...] = dot3((edge_t_hi[...], edge_t_lo[...]), panel)
    outer_decay[...] = dot3(split(outer[...]), decays)

    near_half = pl.ds(first, TILE)
    far_half = pl.ds(pl.multiple_of(TILE - first, TILE), TILE)
    far_pos = iota((TILE, BANDS), 0)
    far_dist = jnp.where(core == 0, far_pos + 1, TILE - far_pos).astype(F32)
    far_rise = jnp.exp(-far_dist / (1 + class_at(iota((TILE, BANDS), 1))).astype(F32))
    any_win = 0.0
    for l in range(CLASSES):
        start = pl.multiple_of(l * PANEL + TILE - first, TILE)
        any_win = any_win + win[pl.ds(start, TILE), :].astype(F32)
    far_rise = split(far_rise * any_win)
    for lb in range(CLASSES):
        filt_rise[lb] = dot3(split(filt[lb, :, far_half]), far_rise)
    outer_rise[...] = dot3(split(outer[:, far_half]), far_rise)
    for copy in mask_copies:
        copy.wait()
    gram[...] = jnp.zeros_like(gram)
    mirror[...] = jnp.zeros_like(mirror)
    for d in range(REACH):
        if SENDS[d] < 0:
            hits = jnp.where(partner_ref[...] == source(d)[0], 1.0, 0.0)
        else:
            hits = jnp.where(got_partner[d] == me, 1.0, 0.0)
        weight = hits[:, 0:1] + hits[:, 1:2]
        for r in range(2):
            marks = got_mask[d, :, lanes_of(near[r])].astype(F32) * weight
            row_marks[d, r] = down(marks, BLOCK)

    def summed(p):
        r, c = pack[p]
        out = 0.0
        for d in range(REACH):
            cols = got_mask[d, :, lanes_of(c)].astype(F32)
            out = out + got[d, p] * row_marks[d, r] * cols
        return out

    def summed_square(p, n):
        r, c = pack[p]
        top = low = 0.0
        for d in range(REACH):
            cols = got_mask[d, :, lanes_of(c)].astype(F32)
            low_cols = jnp.where(lower[:1], pltpu.roll(cols, HALF, 1), cols)
            marks = row_marks[d, r]
            low_marks = jnp.where(lower, marks[HALF : HALF + HALF // 2], marks[HALF + HALF // 2 :])
            top = top + got[d, p, :HALF] * marks[:HALF] * cols
            low = low + got_low[d, n] * low_marks * low_cols
        square = jnp.concatenate((top, pltpu.roll(low, HALF, 1), low), axis=0)
        row, lane_at = iota((BLOCK, BLOCK), 0), iota((BLOCK, BLOCK), 1)
        return jnp.where((row >= HALF) & (lane_at < HALF), jnp.transpose(square), square)

    def filtered(rows, l):
        square = slice(l * PANEL, l * PANEL + TILE)
        return dot3(rows, (toep_hi[:TILE, square], toep_lo[:TILE, square]))

    far_copy = pltpu.make_async_remote_copy(
        src_ref=far_sum, dst_ref=got_far,
        send_sem=far_sem.at[0], recv_sem=far_sem.at[1], device_id=sibling, device_id_type=MESH,
    )
    for copy in copies[0]:
        copy.wait_recv()
    for r in range(2):
        far_sum[r] = summed(r)
    far_copy.start()
    far_copy.wait_recv()
    far_block = 2 - 2 * core
    for r in range(2):
        for block, value in (
            (far[r], far_sum[r]), (missing[r], jnp.transpose(got_far[missing_slot[r]]))
        ):
            lanes_at = pl.ds(pl.multiple_of(BLOCK * (block - far_block), BLOCK), BLOCK)
            hi, lo = split(value)
            rows_hi[r * BLOCK : (r + 1) * BLOCK, lanes_at] = hi
            rows_lo[r * BLOCK : (r + 1) * BLOCK, lanes_at] = lo
    rows = (rows_hi[...], rows_lo[...])
    far_edges[...] = dot3(rows, (edge_hi[far_half, :], edge_lo[far_half, :]))
    far_gram = dot3((decay_t_hi[:, near_half], decay_t_lo[:, near_half]), rows)
    gram_hi, gram_lo = split(far_gram)
    stack = tuple(jnp.concatenate(pair, axis=0) for pair in ((rows[0], gram_hi), (rows[1], gram_lo)))
    for l in range(CLASSES):
        far_out[:, l * TILE : (l + 1) * TILE] = filtered(stack, l)
    inside_all = jnp.concatenate([win_t[lb, :, near_half] for lb in range(CLASSES)], axis=1)
    for la in range(CLASSES):
        out = far_out[:ROWS, la * TILE : (la + 1) * TILE]
        hi, lo = split(
            jnp.concatenate([out * filt[lb, :, far_half] for lb in range(la, CLASSES)], axis=0)
        )
        above = inside_all[:, la * ROWS :]
        rim = far_out[ROWS:, la * TILE : (la + 1) * TILE] * outer[:, far_half]
        box = mm(above, hi) + mm(above, lo) - (rim[:BANDS] + rim[BANDS:])
        boxes[:, la * TILE : (la + 1) * TILE] = box
    far_fisher = jnp.zeros((BANDS, BANDS), F32)
    for la in range(CLASSES):
        hi, lo = split(boxes[:, la * TILE : (la + 1) * TILE])
        channels = win[pl.ds(pl.multiple_of(la * PANEL + TILE - first, TILE), TILE), :]
        far_fisher = far_fisher + (mm(hi, channels) + mm(lo, channels))
    total[...] = far_fisher

    in_low = core == 0
    tile_lane = iota((1, TILE), 1).astype(F32)
    rises = []
    for l in range(CLASSES):
        to_low = jnp.exp((tile_lane - TILE) * (1.0 / (1 + l)))
        to_high = jnp.exp((tile_lane + 1.0) * (-1.0 / (1 + l)))
        rises.append(jnp.where(in_low, to_low, to_high))
    for k in range(2):
        y0 = k * BLOCK
        for copy in copies[k + 1]:
            copy.wait_recv()
        if k == 0:
            corner = summed(3)
            blocks = (summed_square(2, 0), corner)
            turned_corner[...] = jnp.transpose(corner)
        else:
            blocks = (turned_corner[...], summed_square(4, 1))
        rows = split(jnp.concatenate(blocks, axis=1))
        here = pl.ds(pl.multiple_of(first + y0, BLOCK), BLOCK)
        decay_t = (decay_t_hi[:, here], decay_t_lo[:, here])
        edges = far_edges[y0 : y0 + BLOCK, :] + dot3(rows, (edge_hi[near_half, :], edge_lo[near_half, :]))
        mirror[...] += dot3(decay_t, split(edges))
        gram[...] += dot3(decay_t, rows)
        stack = rows
        if k == 1:
            near_gram = split(gram[...])
            stack = tuple(jnp.concatenate((a, b), axis=0) for a, b in zip(rows, near_gram))
        rims = []
        for lb in range(CLASSES):
            rim = edges[:, : 2 * BANDS] * filt_edge[lb, y0 : y0 + BLOCK, :]
            spilt = edges[:, 3 * BANDS :] * filt_rise[lb, y0 : y0 + BLOCK, :]
            rims.append(rim[:, :BANDS] + rim[:, BANDS:] - spilt)
        inside = jnp.concatenate([win_t[lb, :, here] for lb in range(CLASSES)], axis=1)
        hi, lo = split(jnp.concatenate(rims, axis=0))
        total[...] -= mm(inside, hi) + mm(inside, lo)
        for la in range(CLASSES):
            near_out = filtered(stack, la)
            above = inside[:, la * BLOCK :]
            step_up = rises[la]
            lane_col = 2 * BANDS + 2 * la
            out = near_out[:BLOCK] + edges[:, lane_col : lane_col + 1] * step_up
            hi, lo = split(
                jnp.concatenate(
                    [out * filt[lb, y0 : y0 + BLOCK, near_half] for lb in range(la, CLASSES)], axis=0
                )
            )
            box = mm(above, hi) + mm(above, lo)
            span = slice(la * TILE, (la + 1) * TILE)
            if k == 0:
                boxes[:, span] = box
            else:
                rim = near_out[BLOCK:] + mirror[:, lane_col : lane_col + 1] * step_up
                rim = rim * outer[:, near_half]
                boxes[:, span] += box - (rim[:BANDS] + rim[BANDS:])
    fisher = total[...]
    for la in range(CLASSES):
        hi, lo = split(boxes[:, la * TILE : (la + 1) * TILE])
        channels = win[pl.ds(pl.multiple_of(la * PANEL + first, TILE), TILE), :]
        fisher = fisher + (mm(hi, channels) + mm(lo, channels))
    over = mirror[:, 3 * BANDS :] * outer_rise[...]
    fisher = fisher - (over[:BANDS] + over[BANDS:])
    four = mirror[:, : 2 * BANDS] * outer_decay[...]
    fisher = fisher + (four[:BANDS, :BANDS] + four[:BANDS, BANDS:])
    fisher = fisher + (four[BANDS:, :BANDS] + four[BANDS:, BANDS:])
    row_class = class_at(iota((BANDS, BANDS), 0))
    col_class = class_at(iota((BANDS, BANDS), 1))
    kept = jnp.where(col_class <= row_class, fisher * SCALE, 0.0)
    wide = jnp.concatenate([kept, jnp.zeros_like(kept)], axis=1)
    turned_over = jnp.transpose(jnp.concatenate([wide, jnp.zeros_like(wide)], axis=0))
    fisher = kept + jnp.where(col_class > row_class, turned_over[:BANDS, :BANDS], 0.0)

    placed = jnp.concatenate([fisher[: BANDS // 2], fisher[BANDS // 2 :]], axis=1)
    for j in range(16):
        sum_xy[j] = placed[2 * j : 2 * j + 2]

    xy_copies = []
    for e in range(1, 16):
        copy = pltpu.make_async_remote_copy(
            src_ref=sum_xy.at[(plane + e) % 16], dst_ref=got_xy.at[e - 1],
            send_sem=xy_sem.at[0, e - 1], recv_sem=xy_sem.at[1, e - 1],
            device_id=plane_peer(e), device_id_type=MESH,
        )
        copy.start()
        xy_copies.append(copy)
    tile = sum_xy[plane]
    for e in range(15):
        xy_copies[e].wait_recv()
        tile = tile + got_xy[e]
    sum_z[0] = tile[0:1]
    sum_z[1] = tile[1:2]
    z_copies = []
    for e in range(1, 8):
        copy = pltpu.make_async_remote_copy(
            src_ref=sum_z.at[(spot + e) % 8 // 4], dst_ref=got_z.at[e - 1],
            send_sem=z_sem.at[0, e - 1], recv_sem=z_sem.at[1, e - 1],
            device_id=z_peer(e), device_id_type=MESH,
        )
        copy.start()
        z_copies.append(copy)
    mine = jnp.where(pos_z == 0, tile[0:1], tile[1:2])
    halves = [jnp.where(half == h, mine, 0.0) for h in range(2)]
    for e in range(7):
        z_copies[e].wait_recv()
        from_half = ((spot + 7 - e) % 8 % 4) // 2
        for h in range(2):
            halves[h] = halves[h] + jnp.where(from_half == h, got_z[e], 0.0)
    lanes = iota((16, 128), 1)
    band = 16 * part + iota((16, 128), 0)
    band = 32 * (band % 2) + 2 * (band // 2 % 16) + band // 32
    for h in range(2):
        line = jnp.broadcast_to(halves[h], (16, 128))
        for side in range(2):
            one = jnp.where(lanes == band + side * BANDS, line, 0.0)
            out_ref[h, :, side : side + 1] = jnp.sum(one, axis=1, keepdims=True)

    for copy in copies[0] + copies[1] + copies[2] + [far_copy] + xy_copies + z_copies:
        copy.wait_send()


def body(*args):
    vmem = pltpu.VMEM
    dma = pltpu.SemaphoreType.DMA
    return pl.pallas_call(
        body_kernel,
        out_shape=jax.ShapeDtypeStruct((2, 16, 2), F32),
        in_specs=[
            pl.BlockSpec(memory_space=pltpu.HBM),
            pl.BlockSpec(memory_space=pltpu.HBM),
            pl.BlockSpec(memory_space=pltpu.HBM),
            pl.BlockSpec(memory_space=pltpu.HBM),
        ],
        out_specs=pl.BlockSpec(memory_space=pltpu.VMEM),
        scratch_shapes=[
            vmem((1, 2 * PANEL), jnp.int32),
            vmem((1, 2), jnp.int32),
            vmem((2, BANDS), jnp.int32),
            vmem((PANEL, PANEL), F32),
            vmem((5, BLOCK, BLOCK), F32),
            vmem((2, HALF // 2, BLOCK), F32),
            vmem((REACH, 5, BLOCK, BLOCK), F32),
            vmem((REACH, 2, HALF // 2, BLOCK), F32),
            vmem((REACH, 1, 2 * PANEL), jnp.int32),
            vmem((REACH, 1, 2), jnp.int32),
            vmem((REACH, 2, BLOCK, BLOCK), F32),
            vmem((2, BLOCK, BLOCK), F32),
            vmem((2, BLOCK, BLOCK), F32),
            vmem((ROWS, 4 * BANDS), F32),
            vmem((ROWS + 2 * BANDS, CLASSES * TILE), F32),
            vmem((CLASSES, ROWS, BANDS), F32),
            vmem((2 * BANDS, BANDS), F32),
            vmem((BLOCK, BLOCK), F32),
            vmem((ROWS, TILE), BF16),
            vmem((ROWS, TILE), BF16),
            vmem((PANEL, CLASSES * PANEL), BF16),
            vmem((PANEL, CLASSES * PANEL), BF16),
            vmem((PANEL, 4 * BANDS), BF16),
            vmem((PANEL, 4 * BANDS), BF16),
            vmem((CLASSES * PANEL, BANDS), BF16),
            vmem((PANEL, 2 * BANDS), BF16),
            vmem((PANEL, 2 * BANDS), BF16),
            vmem((2 * BANDS, PANEL), BF16),
            vmem((2 * BANDS, PANEL), BF16),
            vmem((2 * BANDS, PANEL), BF16),
            vmem((2 * BANDS, PANEL), BF16),
            vmem((CLASSES, BANDS, PANEL), BF16),
            vmem((PANEL, PANEL), BF16),
            vmem((PANEL, PANEL), BF16),
            vmem((CLASSES, ROWS, PANEL), F32),
            vmem((CLASSES, ROWS, 2 * BANDS), F32),
            vmem((2 * BANDS, PANEL), F32),
            vmem((2 * BANDS, 2 * BANDS), F32),
            vmem((BANDS, CLASSES * TILE), F32),
            vmem((2 * BANDS, TILE), F32),
            vmem((BANDS, BANDS), F32),
            vmem((2 * BANDS, 4 * BANDS), F32),
            vmem((16, 2, 128), F32),
            vmem((15, 2, 128), F32),
            vmem((2, 1, 128), F32),
            vmem((7, 1, 128), F32),
            dma((REACH, 6)),
            dma((REACH, 6)),
            dma((2, REACH)),
            dma((2, REACH)),
            dma((2,)),
            dma((2,)),
            dma((9,)),
            dma((2, 15)),
            dma((2, 7)),
        ],
        compiler_params=pltpu.CompilerParams(
            collective_id=0, has_side_effects=True, vmem_limit_bytes=48 * 1024 * 1024
        ),
    )(*(pltpu.with_memory_space_constraint(x, pltpu.HBM) for x in args))


def solution(mesh):
    placed = (P("bl", "bp", None), P("bl", None), P("bl", None), P())
    return jax.shard_map(
        body, mesh=mesh, in_specs=placed, out_specs=P(None, "bp", "bl"), check_vma=False
    )
```
